32 devices in a mesh: dp: 8 (over y, x, core), mp: 4 (over z).
Axes of the slice: x: 2, y: 2, z: 4, core: 2. Of those that a mesh axis runs over, the one named last changes fastest.
Arguments:
- doc_ids: int32 [8, 512], P('dp'), may hold values from 0 to 128255
- doc_lengths: int32 [8], P('dp'), may hold values from 128 to 512
- activations: bfloat16 [4096, 4096], P('dp'), may hold values from -6 to 6
- out_grads: bfloat16 [4096, 14336], P('dp'), may hold values from -0.29882812 to 0.29882812
- input_basis: bfloat16 [4096, 2048], P(None, 'mp'), may hold values from -0.09375 to 0.09375
- output_basis: bfloat16 [14336, 7168], P('dp', 'mp'), may hold values from -0.046875 to 0.046875
- eigenvalues: bfloat16 [2048, 7168], P(None, 'mp'), may hold values from 0.5 to 50
- query_left: bfloat16 [32, 32, 2048], P('dp'), may hold values from -0.125 to 0.125
- query_right: bfloat16 [32, 32, 7168], P('dp', None, 'mp'), may hold values from -0.0625 to 0.0625
Outputs:
- scores: float32 [8, 32], P('dp')
The draws below stay inside these ranges and needn't reach their ends.
Inputs may be any that keep to these rules, and one draw needn't show every extreme that they name: `doc_lengths`: the live tokens are the first ones of each document.
All inputs are finite; a program needn't handle non-finite values.
Results may differ from the reference program's by a relative error of at most 0.023.
Values may be sent and summed in bfloat16 or wider, within the bound.
A program may use at most 192 MiB of HBM per device.

```python
import math
import jax
import jax.numpy as jnp
import numpy as np
from jax import lax

D = 4096
FF = 14336
VOCAB = 128256
KIN = 2048
KOUT = 7168
RANK = 32
DOC_LEN = 512
DOCS = 8
QUERIES = 32
TOKENS = 4096
N_DP = 8


def plant(drawn, stream_key, least, largest):
    dims = drawn.shape
    place = [jax.random.randint(jax.random.fold_in(stream_key, axis), (), 0, dims[axis]) for axis in range(len(dims))]
    drawn = drawn.at[tuple(place)].set(least)
    longest = dims.index(max(dims))
    place[longest] = (place[longest] + 1) % dims[longest]
    return drawn.at[tuple(place)].set(largest)


def levels(stream_key, dims, pieces, low, top_value):
    loudness = 1.0
    for axis_at, parts in pieces:
        draws = jax.random.uniform(jax.random.fold_in(jax.random.fold_in(stream_key, 6), axis_at), (parts,), jnp.float32, low / len(pieces), top_value / len(pieces))
        loudness = loudness * jnp.repeat(jnp.exp(draws), dims[axis_at] // parts).reshape((-1,) + (1,) * (len(dims) - 1 - axis_at))
    return loudness


def skewed_wide(stream_key, shape, number_of, skew):
    weights = [min(1 << octave, number_of + 1 - (1 << octave)) * (1 << 20) // math.isqrt((1 << octave) ** skew) + 1 for octave in range((number_of + 1).bit_length()) if 1 << octave <= number_of]
    scale = 1 + sum(weights) // (1 << 30)
    table = np.cumsum(np.array([max(1, weight // scale) for weight in weights]))
    pick = jax.random.randint(jax.random.fold_in(stream_key, 1), shape, 0, int(table[len(weights) - 1]))
    start = jnp.left_shift(1, jnp.searchsorted(jnp.asarray(table, jnp.int32), pick, side="right").astype(jnp.int32))
    grade = start - 1 + jax.random.randint(jax.random.fold_in(stream_key, 4), shape, 0, 1 << 30) % jnp.minimum(start, number_of + 1 - start)
    return jax.random.permutation(jax.random.fold_in(stream_key, 2), number_of)[grade].astype(jnp.int32)


def gaussian(own_key, extent, scale, reach, shards=(), held_as=jnp.bfloat16):
    result = jax.random.normal(own_key, extent, jnp.float32) * scale
    if len(shards) > 0:
        result = levels(own_key, extent, shards, -0.22, 0.18) * result
    return jnp.clip(result, min=-reach, max=reach).astype(held_as)


def setup_inputs(seed: int = 0) -> dict:
    key_of = jax.random.split(jax.random.key(seed), 10)
    doc_ids = plant(skewed_wide(key_of[0], (DOCS, DOC_LEN), VOCAB, 2), jax.random.fold_in(key_of[0], 3), 0, VOCAB - 1).astype(jnp.int32)
    doc_lengths = plant(jax.random.randint(key_of[1], (DOCS,), DOC_LEN // 4, DOC_LEN + 1), jax.random.fold_in(key_of[1], 1), DOC_LEN // 4, DOC_LEN).astype(jnp.int32)
    activations = gaussian(key_of[2], (TOKENS, D), 1.0, 6.0, ((0, 8),))
    out_grads = gaussian(key_of[3], (TOKENS, FF), 0.05, 0.29882812, ((0, 8),))
    input_basis = gaussian(key_of[4], (D, KIN), D ** -0.5, 0.09375, ((1, 4),))
    output_basis = gaussian(key_of[5], (FF, KOUT), FF ** -0.5, 0.046875, ((0, 8), (1, 4)))
    eigenvalues = jnp.clip(jnp.exp(math.log(50.0) - 4.6051702 * jax.random.uniform(key_of[6], (KIN, KOUT), jnp.float32) ** levels(key_of[6], (KIN, KOUT), ((1, 4),), -0.2, 0.2)), 0.5, 50.0).astype(jnp.bfloat16)
    query_left = gaussian(key_of[7], (QUERIES, RANK, KIN), KIN ** -0.5, 0.125, ((0, 8),))
    query_right = gaussian(key_of[8], (QUERIES, RANK, KOUT), KOUT ** -0.5, 0.0625, ((0, 8), (2, 4)))
    return {"doc_ids": doc_ids, "doc_lengths": doc_lengths, "activations": activations, "out_grads": out_grads, "input_basis": input_basis, "output_basis": output_basis, "eigenvalues": eigenvalues, "query_left": query_left, "query_right": query_right}


damping = 0.5


def token_weights(doc_ids, doc_lengths):
    positions = jnp.arange(doc_ids.shape[1], dtype=jnp.int32)
    active = positions[None, :] < doc_lengths[:, None]
    matches = (doc_ids[:, :, None] == doc_ids[:, None, :]) & active[:, None, :]
    repeats = jnp.sum(matches.astype(jnp.float32), axis=2)
    return jnp.where(active, 1.0 / jnp.maximum(repeats, 1.0), 0.0).astype(jnp.float32)


def reference(doc_ids, doc_lengths, activations, out_grads, input_basis, output_basis, eigenvalues, query_left, query_right):
    rotated_in = jnp.dot(activations, input_basis, preferred_element_type=jnp.float32).astype(jnp.bfloat16)
    width = FF // N_DP
    summed = jnp.zeros((TOKENS, KOUT), jnp.float32)
    for member in range(N_DP):
        partial_value = jnp.dot(out_grads[:, member * width:(member + 1) * width], output_basis[member * width:(member + 1) * width], preferred_element_type=jnp.float32)
        summed = summed + lax.optimization_barrier(partial_value.astype(jnp.bfloat16)).astype(jnp.float32)
    rotated_out = summed.astype(jnp.bfloat16)
    weights = token_weights(doc_ids, doc_lengths)
    left_rows = query_left.reshape(QUERIES * RANK, KIN)
    right_rows = query_right.reshape(QUERIES * RANK, KOUT).astype(jnp.float32)
    denominator = eigenvalues.astype(jnp.float32) + damping

    def per_document(doc_index):
        first = doc_index * DOC_LEN
        acts_doc = lax.dynamic_slice_in_dim(rotated_in, first, DOC_LEN, 0)
        grads_doc = lax.dynamic_slice_in_dim(rotated_out, first, DOC_LEN, 0)
        weight_doc = lax.dynamic_index_in_dim(weights, doc_index, 0, keepdims=False)
        scaled = (weight_doc[:, None] * grads_doc.astype(jnp.float32)).astype(jnp.bfloat16)
        gradient = jnp.dot(acts_doc.T, scaled, preferred_element_type=jnp.float32)
        conditioned = (gradient / denominator).astype(jnp.bfloat16)
        mixture = jnp.dot(left_rows, conditioned, preferred_element_type=jnp.float32)
        return jnp.sum((mixture * right_rows).reshape(QUERIES, RANK * KOUT), axis=1)

    return lax.map(per_document, jnp.arange(DOCS, dtype=jnp.int32))
```

```python
import functools

import jax
import jax.numpy as jnp
from jax import lax
from jax.experimental import pallas as pl
from jax.experimental.pallas import tpu as pltpu
from jax.sharding import PartitionSpec as P

damping = 0.5
LAG = 3


def piece_width(columns):
    return 256 if columns % 256 == 0 else 128


def kernel(
    n_dp,
    n_mp,
    ids_col,
    ids_row,
    length,
    acts,
    grads,
    in_basis,
    out_basis,
    eigen,
    q_left,
    q_right,
    out,
    basis,
    own_g,
    peer_g,
    rin,
    left,
    right,
    eig,
    part_out,
    part_in,
    own_out,
    act_buf,
    inb_buf,
    acc,
    cond,
    weight,
    sums,
    gathered,
    load_sem,
    chunk_sem,
    eig_sem,
    bx_s,
    bx_r,
    bd_s,
    bd_r,
    bf_s,
    bf_r,
    gs_s,
    gs_r,
    gd_s,
    gd_r,
    zr_s,
    zr_r,
    zl_s,
    zl_r,
    rz_s,
    rz_r,
    qx_s,
    qx_r,
    qy_s,
    qy_r,
    qd_s,
    qd_r,
    ss_s,
    ss_r,
    sc_s,
    sc_r,
):
    groups = n_dp // 4
    dp, mp = lax.axis_index("dp"), lax.axis_index("mp")
    group, place = lax.div(dp, 4), lax.rem(dp, 4)
    places = (place, place + 1 - 2 * lax.rem(place, 2), lax.rem(place + 2, 4), 3 - place)

    tokens = grads.shape[0]
    depth, cols = out_basis.shape
    width = piece_width(cols)
    pieces = cols // width
    in_cols = in_basis.shape[1]
    kin = rin.shape[0]
    q_rows = q_left.shape[0]
    shared = (tokens * 3 // 4) // n_mp // 16 * 16
    direct = tokens - shared * n_mp

    def at_dp(index):
        return (index, mp)

    def at_mp(index):
        return (dp, index)

    partner = at_dp(group * 4 + places[1])
    across = at_dp(group * 4 + places[2])

    def group_at(s):
        return lax.rem(group + s, groups)

    def peer(s):
        return at_dp(group_at(s) * 4 + place)

    def remote(src, dst, send, recv, device):
        return pltpu.make_async_remote_copy(
            src_ref=src,
            dst_ref=dst,
            send_sem=send,
            recv_sem=recv,
            device_id=device,
            device_id_type=pl.DeviceIdType.MESH,
        )

    barrier = pltpu.get_barrier_semaphore()
    friends = [partner, across]
    friends += [peer(s) for s in range(1, groups)]
    friends += [at_mp(lax.rem(mp + m, n_mp)) for m in range(1, n_mp)]
    for friend in friends:
        pl.semaphore_signal(barrier, inc=1, device_id=friend, device_id_type=pl.DeviceIdType.MESH)
    pl.semaphore_wait(barrier, len(friends))

    sends = []

    def go(copy):
        copy.start()
        sends.append(copy)

    def piece(p):
        return pl.ds(pl.multiple_of(p * width, width), width)

    def rows_of(index):
        return pl.ds(pl.multiple_of(index * q_rows, q_rows), q_rows)

    def basis_across(p):
        return remote(
            out_basis.at[:, piece(p)],
            basis.at[pl.ds(2 * depth, depth), piece(p)],
            bx_s.at[p],
            bx_r.at[p],
            across,
        )

    def basis_forward(p):
        return remote(
            basis.at[pl.ds(2 * depth, depth), piece(p)],
            basis.at[pl.ds(3 * depth, depth), piece(p)],
            bf_s.at[p],
            bf_r.at[p],
            partner,
        )

    basis_partner = remote(
        out_basis, basis.at[pl.ds(depth, depth), :], bd_s.at[0], bd_r.at[0], partner
    )

    def grads_over(s, q, first, rows, send, recv):
        start = (group_at(s) * 4 + places[q]) * depth
        return remote(
            grads.at[pl.ds(first, rows), pl.ds(pl.multiple_of(start, 128), depth)],
            peer_g.at[s - 1, pl.ds(first, rows), pl.ds(q * depth, depth)],
            send,
            recv,
            peer(s),
        )

    def share_first(plane):
        return pl.multiple_of(direct + plane * shared, 16)

    chunks = [(s, q) for s in range(1, groups) for q in range(4)]

    def grads_shared(e):
        s, q = chunks[e]
        return grads_over(s, q, share_first(mp), shared, gs_s.at[e], gs_r.at[e])

    def grads_direct(e):
        s, q = chunks[e]
        return grads_over(s, q, 0, direct, gd_s.at[e], gd_r.at[e])

    def share(e, plane):
        s, q = chunks[e]
        return peer_g.at[s - 1, pl.ds(share_first(plane), shared), pl.ds(q * depth, depth)]

    def relay_up(e, r):
        ref = share(e, mp - r)
        return remote(ref, ref, zr_s.at[e, r], zr_r.at[e, r + 1], at_mp(mp + 1))

    def relay_down(e, r):
        ref = share(e, mp + r)
        return remote(ref, ref, zl_s.at[e, r], zl_r.at[e, r + 1], at_mp(mp - 1))

    def from_below(e, r):
        ref = share(e, mp - r)
        return remote(ref, ref, zr_s.at[e, r], zr_r.at[e, r], at_mp(mp - 1))

    def from_above(e, r):
        ref = share(e, mp + r)
        return remote(ref, ref, zl_s.at[e, r], zl_r.at[e, r], at_mp(mp + 1))

    tables = ((q_left, left), (q_right, right))
    mine = group * 4 + place
    theirs = group * 4 + places[2]

    def query_across(k):
        source, table = tables[k]
        return remote(source, table.at[rows_of(mine), :], qx_s.at[k], qx_r.at[k], across)

    def query_arrived_across(k):
        source, table = tables[k]
        return remote(source, table.at[rows_of(theirs), :], qx_s.at[k], qx_r.at[k], across)

    def query_over(s, j, k):
        source, table = tables[k]
        slot = ((s - 1) * 2 + j) * 2 + k
        rows = table.at[rows_of((mine, theirs)[j]), :]
        return remote(source if j == 0 else rows, rows, qy_s.at[slot], qy_r.at[slot], peer(s))

    def query_arrived_over(s, j, k):
        table = tables[k][1]
        slot = ((s - 1) * 2 + j) * 2 + k
        origin = group_at(groups - s) * 4 + (place, places[2])[j]
        rows = table.at[rows_of(origin), :]
        return remote(rows, rows, qy_s.at[slot], qy_r.at[slot], peer(groups - s))

    def query_partner(s, j, k):
        source, table = tables[k]
        slot = (s * 2 + j) * 2 + k
        origin = group_at(groups - s) * 4 + (place, places[2])[j]
        rows = table.at[rows_of(origin), :]
        first = source if s == 0 and j == 0 else rows
        return remote(first, rows, qd_s.at[slot], qd_r.at[slot], partner)

    def query_arrived_partner(s, j, k):
        table = tables[k][1]
        slot = (s * 2 + j) * 2 + k
        origin = group_at(groups - s) * 4 + (places[1], places[3])[j]
        rows = table.at[rows_of(origin), :]
        return remote(rows, rows, qd_s.at[slot], qd_r.at[slot], partner)

    for p in range(min(2, pieces)):
        go(basis_across(p))
    for e in range(len(chunks)):
        go(grads_shared(e))
    for k in range(2):
        go(query_across(k))
    for p in range(2, pieces):
        go(basis_across(p))
    go(basis_partner)
    for k in range(2):
        go(query_partner(0, 0, k))
    for e in range(len(chunks)):
        go(grads_direct(e))
    for s in range(1, groups):
        for k in range(2):
            go(query_over(s, 0, k))

    k_chunks = acts.shape[1] // act_buf.shape[2]
    k_size = act_buf.shape[2]

    def load_chunk(i):
        slot = i % 2
        return (
            pltpu.make_async_copy(
                acts.at[:, pl.ds(i * k_size, k_size)], act_buf.at[slot], chunk_sem.at[slot, 0]
            ),
            pltpu.make_async_copy(
                in_basis.at[pl.ds(i * k_size, k_size), :], inb_buf.at[slot], chunk_sem.at[slot, 1]
            ),
        )

    for copy in load_chunk(0):
        copy.start()
    loads = [pltpu.make_async_copy(out_basis, basis.at[pl.ds(0, depth), :], load_sem.at[0])]
    for q in range(4):
        start = (group * 4 + places[q]) * depth
        loads.append(
            pltpu.make_async_copy(
                grads.at[:, pl.ds(pl.multiple_of(start, 128), depth)],
                own_g.at[:, pl.ds(q * depth, depth)],
                load_sem.at[1 + q],
            )
        )
    for k in range(2):
        loads.append(
            pltpu.make_async_copy(tables[k][0], tables[k][1].at[rows_of(mine), :], load_sem.at[5 + k])
        )
    for copy in loads:
        copy.start()

    def load_eig(p):
        slot = lax.rem(p, 2)
        return pltpu.make_async_copy(eigen.at[:, piece(p)], eig.at[slot], eig_sem.at[slot])

    load_eig(0).start()

    for i in range(k_chunks):
        if i + 1 < k_chunks:
            for copy in load_chunk(i + 1):
                copy.start()
        for copy in load_chunk(i):
            copy.wait()
        term = jnp.dot(act_buf[i % 2], inb_buf[i % 2], preferred_element_type=jnp.float32)
        if i == 0:
            acc[:, :in_cols] = term
        else:
            acc[:, :in_cols] += term
    rin_rows = pl.ds(pl.multiple_of(mp * in_cols, in_cols), in_cols)
    rin[rin_rows, :] = jnp.transpose(acc[:, :in_cols]).astype(jnp.bfloat16)

    live = length[0, 0]
    active_row = lax.broadcasted_iota(jnp.int32, (1, tokens), 1) < live
    active_col = lax.broadcasted_iota(jnp.int32, (tokens, 1), 0) < live
    same = (ids_col[...] == ids_row[...]) & active_row
    repeats = jnp.sum(jnp.where(same, 1.0, 0.0), axis=1, keepdims=True)
    weight[...] = jnp.where(active_col, 1.0 / jnp.maximum(repeats, 1.0), 0.0)
    sums[...] = jnp.zeros_like(sums)

    def up_if(r):
        return (mp >= r) & (mp < n_mp - 1)

    def down_if(r):
        return (mp + r <= n_mp - 1) & (mp > 0)

    for step in range(len(chunks) + n_mp - 1):
        if step < len(chunks):
            grads_shared(step).wait_recv()
        for r in range(n_mp):
            e = step - r
            if not 0 <= e < len(chunks):
                continue

            @pl.when(up_if(r))
            def _():
                if r > 0:
                    from_below(e, r).wait_recv()
                relay_up(e, r).start()

            @pl.when(down_if(r))
            def _():
                if r > 0:
                    from_above(e, r).wait_recv()
                relay_down(e, r).start()

    def rin_over(m):
        ref = rin.at[rin_rows, :]
        return remote(ref, ref, rz_s.at[m], rz_r.at[m], at_mp(lax.rem(mp + m, n_mp)))

    def rin_arrived(m):
        source = lax.rem(mp + n_mp - m, n_mp)
        ref = rin.at[pl.ds(pl.multiple_of(source * in_cols, in_cols), in_cols), :]
        return remote(ref, ref, rz_s.at[m], rz_r.at[m], at_mp(source))

    for m in range(1, n_mp):
        go(rin_over(m))

    for k in range(2):
        query_arrived_across(k).wait_recv()
        for s in range(1, groups):
            go(query_over(s, 1, k))
        go(query_partner(0, 1, k))

    for copy in loads:
        copy.wait()
    basis_partner.wait_recv()
    for e in range(len(chunks)):
        grads_direct(e).wait_recv()
        for r in range(1, n_mp):

            @pl.when((mp >= r) & (mp == n_mp - 1))
            def _():
                from_below(e, r).wait_recv()

            @pl.when((mp + r <= n_mp - 1) & (mp == 0))
            def _():
                from_above(e, r).wait_recv()

    def part_over(s, p):
        return remote(
            part_out.at[s - 1, :, piece(p)],
            part_in.at[s - 1, :, piece(p)],
            ss_s.at[s - 1, p],
            ss_r.at[s - 1, p],
            peer(groups - s),
        )

    rows_from = [peer_g.at[s - 1] for s in range(1, groups)] + [own_g]

    def rotate(p):
        def term(rows, first, count):
            k = pl.ds(first * depth, count * depth)
            return jnp.dot(rows[:, k], basis[k, piece(p)], preferred_element_type=jnp.float32)

        def part(j):
            return pl.ds(j * width, width)

        for j, rows in enumerate(rows_from):
            acc[:, part(j)] = term(rows, 0, 2)
        basis_across(p).wait_recv()
        basis_forward(p).start()
        for j, rows in enumerate(rows_from):
            acc[:, part(j)] += term(rows, 2, 1)
        basis_forward(p).wait_recv()
        for j, rows in enumerate(rows_from):
            total = acc[:, part(j)] + term(rows, 3, 1)
            if j < groups - 1:
                part_out[j, :, piece(p)] = total.astype(jnp.bfloat16)
                part_over(j + 1, p).start()
            else:
                own_out[:, piece(p)] = total.astype(jnp.bfloat16)

    def score(p):
        @pl.when(p == 0)
        def _():
            for m in range(1, n_mp):
                rin_arrived(m).wait_recv()
            for s in range(1, groups):
                for j in range(2):
                    for k in range(2):
                        query_arrived_over(s, j, k).wait_recv()
                        query_partner(s, j, k).start()
            for s in range(groups):
                for j in range(2):
                    for k in range(2):
                        query_arrived_partner(s, j, k).wait_recv()

        load_eig(p).wait()

        @pl.when(p + 1 < pieces)
        def _():
            load_eig(p + 1).start()

        total = own_out[:, piece(p)].astype(jnp.float32)
        for s in range(1, groups):
            part_over(s, p).wait_recv()
            total = total + part_in[s - 1, :, piece(p)].astype(jnp.float32)
        rotated = total.astype(jnp.bfloat16).astype(jnp.float32)
        scaled = (weight[...] * rotated).astype(jnp.bfloat16)
        slot = lax.rem(p, 2)
        block = 512
        for i in range(0, kin, block):
            gradient = jnp.dot(rin[pl.ds(i, block), :], scaled, preferred_element_type=jnp.float32)
            denominator = eig[slot, pl.ds(i, block), :].astype(jnp.float32) + damping
            cond[pl.ds(i, block), :] = (gradient / denominator).astype(jnp.bfloat16)
        for i in range(0, left.shape[0], block):
            rows = pl.ds(i, block)
            mixture = jnp.dot(left[rows, :], cond[...], preferred_element_type=jnp.float32)
            weighted = mixture * right[rows, piece(p)].astype(jnp.float32)
            folded = weighted[:, :128]
            for c in range(128, width, 128):
                folded = folded + weighted[:, c : c + 128]
            sums[rows, :] += folded

    def step(p, carry):
        @pl.when(p < pieces)
        def _():
            rotate(p)

        @pl.when(p >= LAG)
        def _():
            score(p - LAG)

        return carry

    lax.fori_loop(0, pieces + LAG, step, 0)

    queries, rank = out.shape[0], left.shape[0] // out.shape[0]
    gathered[0] = jnp.sum(sums[...].reshape(queries, rank, 128), axis=1)

    def score_over(m):
        return remote(
            gathered.at[0],
            gathered.at[m],
            sc_s.at[m],
            sc_r.at[m],
            at_mp(lax.rem(mp + m, n_mp)),
        )

    for m in range(1, n_mp):
        go(score_over(m))
    total = gathered[0]
    for m in range(1, n_mp):
        score_over(m).wait_recv()
        total = total + gathered[m]
    out[...] = total

    for copy in sends:
        copy.wait_send()
    for s in range(1, groups):
        for j in range(2):
            for k in range(2):
                query_partner(s, j, k).wait_send()

    def sent(p, carry):
        basis_forward(p).wait_send()
        for s in range(1, groups):
            part_over(s, p).wait_send()
        return carry

    lax.fori_loop(0, pieces, sent, 0)
    for e in range(len(chunks)):
        for r in range(n_mp):

            @pl.when(up_if(r))
            def _():
                relay_up(e, r).wait_send()

            @pl.when(down_if(r))
            def _():
                relay_down(e, r).wait_send()


def per_device(
    n_dp,
    n_mp,
    doc_ids,
    doc_lengths,
    activations,
    out_grads,
    input_basis,
    output_basis,
    eigenvalues,
    query_left,
    query_right,
):
    groups = n_dp // 4
    tokens = out_grads.shape[0]
    depth, cols = output_basis.shape
    kin = eigenvalues.shape[0]
    in_cols = input_basis.shape[1]
    per_block, rank = query_left.shape[:2]
    q_rows = per_block * rank
    queries = n_dp * per_block
    width = piece_width(cols)
    pieces = cols // width
    chunks = (groups - 1) * 4
    k_size = 512
    bf16, f32 = jnp.bfloat16, jnp.float32

    def pair(*shape):
        return [pltpu.SemaphoreType.DMA(shape), pltpu.SemaphoreType.DMA(shape)]

    vmem = pl.BlockSpec(memory_space=pltpu.VMEM)
    hbm = pl.BlockSpec(memory_space=pl.ANY)
    summed = pl.pallas_call(
        functools.partial(kernel, n_dp, n_mp),
        out_shape=jax.ShapeDtypeStruct((queries, 128), f32),
        in_specs=[vmem, vmem, pl.BlockSpec(memory_space=pltpu.SMEM)] + [hbm] * 7,
        out_specs=vmem,
        scratch_shapes=[
            pltpu.VMEM((4 * depth, cols), bf16),
            pltpu.VMEM((tokens, 4 * depth), bf16),
            pltpu.VMEM((groups - 1, tokens, 4 * depth), bf16),
            pltpu.VMEM((kin, tokens), bf16),
            pltpu.VMEM((n_dp * q_rows, kin), bf16),
            pltpu.VMEM((n_dp * q_rows, cols), bf16),
            pltpu.VMEM((2, kin, width), bf16),
            pltpu.VMEM((groups - 1, tokens, cols), bf16),
            pltpu.VMEM((groups - 1, tokens, cols), bf16),
            pltpu.VMEM((tokens, cols), bf16),
            pltpu.VMEM((2, tokens, k_size), bf16),
            pltpu.VMEM((2, k_size, in_cols), bf16),
            pltpu.VMEM((tokens, max(in_cols, groups * width)), f32),
            pltpu.VMEM((kin, width), bf16),
            pltpu.VMEM((tokens, 1), f32),
            pltpu.VMEM((n_dp * q_rows, 128), f32),
            pltpu.VMEM((n_mp, queries, 128), f32),
            pltpu.SemaphoreType.DMA((7,)),
            pltpu.SemaphoreType.DMA((2, 2)),
            pltpu.SemaphoreType.DMA((2,)),
            *pair(pieces),
            *pair(1),
            *pair(pieces),
            *pair(chunks),
            *pair(chunks),
            *pair(chunks, n_mp + 1),
            *pair(chunks, n_mp + 1),
            *pair(n_mp),
            *pair(2),
            *pair((groups - 1) * 4),
            *pair(groups * 4),
            *pair(groups - 1, pieces),
            *pair(n_mp),
        ],
        compiler_params=pltpu.CompilerParams(
            collective_id=0, has_side_effects=True, vmem_limit_bytes=67043328
        ),
    )(
        doc_ids.reshape(tokens, 1),
        doc_ids.reshape(1, tokens),
        doc_lengths.reshape(1, 1),
        activations,
        out_grads,
        input_basis,
        output_basis,
        eigenvalues,
        query_left.reshape(q_rows, kin),
        query_right.reshape(q_rows, cols),
    )
    return jnp.sum(summed, axis=1).reshape(1, queries)


def solution(mesh):
    return jax.shard_map(
        functools.partial(per_device, mesh.shape["dp"], mesh.shape["mp"]),
        mesh=mesh,
        in_specs=(
            P("dp", None),
            P("dp"),
            P("dp", None),
            P("dp", None),
            P(None, "mp"),
            P("dp", "mp"),
            P(None, "mp"),
            P("dp", None, None),
            P("dp", None, "mp"),
        ),
        out_specs=P("dp", None),
        check_vma=False,
    )
```

```python
import functools

import jax
import jax.numpy as jnp
from jax import lax
from jax.experimental import pallas as pl
from jax.experimental.pallas import tpu as pltpu
from jax.sharding import PartitionSpec as P

damping = 0.5
LAG = 3
EARLY = 3


def piece_plan(columns):
    width = 256 if columns % 256 == 0 else 128
    return width, columns // width - 1, [128] * (width // 128)


def kernel(
    n_dp,
    n_mp,
    ids,
    length,
    acts,
    grads,
    in_basis,
    out_basis,
    eigen,
    q_left,
    q_right,
    out,
    basis,
    own_g,
    peer_g,
    rin,
    left,
    right,
    eig,
    part_out,
    part_in,
    own_out,
    act_buf,
    inb_buf,
    acc,
    cond,
    weight,
    sums,
    gathered,
    load_sem,
    chunk_sem,
    eig_sem,
    bx_s,
    bx_r,
    bd_s,
    bd_r,
    bf_s,
    bf_r,
    gs_s,
    gs_r,
    gd_s,
    gd_r,
    zr_s,
    zr_r,
    zl_s,
    zl_r,
    rz_s,
    rz_r,
    qx_s,
    qx_r,
    qy_s,
    qy_r,
    qd_s,
    qd_r,
    ss_s,
    ss_r,
    sc_s,
    sc_r,
):
    groups = n_dp // 4
    dp, mp = lax.axis_index("dp"), lax.axis_index("mp")
    group, place = lax.div(dp, 4), lax.rem(dp, 4)
    places = (place, place + 1 - 2 * lax.rem(place, 2), lax.rem(place + 2, 4), 3 - place)

    tokens = grads.shape[0]
    depth, cols = out_basis.shape
    width, wide, ends = piece_plan(cols)
    pieces = wide + len(ends)
    early = min(EARLY, wide)
    in_cols = in_basis.shape[1]
    kin = rin.shape[0]
    q_rows = q_left.shape[0]
    shared = (tokens * 5 // 8) // n_mp // 16 * 16
    direct = tokens - shared * n_mp

    def at_dp(index):
        return (index, mp)

    def at_mp(index):
        return (dp, index)

    partner = at_dp(group * 4 + places[1])
    across = at_dp(group * 4 + places[2])

    def group_at(s):
        return lax.rem(group + s, groups)

    def peer(s):
        return at_dp(group_at(s) * 4 + place)

    def remote(src, dst, send, recv, device):
        return pltpu.make_async_remote_copy(
            src_ref=src,
            dst_ref=dst,
            send_sem=send,
            recv_sem=recv,
            device_id=device,
            device_id_type=pl.DeviceIdType.MESH,
        )

    barrier = pltpu.get_barrier_semaphore()
    friends = [partner, across]
    friends += [peer(s) for s in range(1, groups)]
    friends += [at_mp(lax.rem(mp + m, n_mp)) for m in range(1, n_mp)]
    for friend in friends:
        pl.semaphore_signal(barrier, inc=1, device_id=friend, device_id_type=pl.DeviceIdType.MESH)
    pl.semaphore_wait(barrier, len(friends))

    sends = []

    def go(copy):
        copy.start()
        sends.append(copy)

    def piece(p, size):
        if size == width and not isinstance(p, int):
            return pl.ds(pl.multiple_of(p * width, width), width)
        return pl.ds(p * width if p < wide else wide * width + (p - wide) * 128, size)

    def size_of(p):
        return width if p < wide else ends[p - wide]

    def rows_of(index):
        return pl.ds(pl.multiple_of(index * q_rows, q_rows), q_rows)

    def basis_across(p, size):
        return remote(
            out_basis.at[:, piece(p, size)],
            basis.at[pl.ds(2 * depth, depth), piece(p, size)],
            bx_s.at[p],
            bx_r.at[p],
            across,
        )

    def basis_forward(p, size):
        return remote(
            basis.at[pl.ds(2 * depth, depth), piece(p, size)],
            basis.at[pl.ds(3 * depth, depth), piece(p, size)],
            bf_s.at[p],
            bf_r.at[p],
            partner,
        )

    basis_partner = remote(
        out_basis, basis.at[pl.ds(depth, depth), :], bd_s.at[0], bd_r.at[0], partner
    )

    def grads_over(s, q, first, rows, send, recv):
        start = (group_at(s) * 4 + places[q]) * depth
        return remote(
            grads.at[pl.ds(first, rows), pl.ds(pl.multiple_of(start, 128), depth)],
            peer_g.at[s - 1, pl.ds(first, rows), pl.ds(q * depth, depth)],
            send,
            recv,
            peer(s),
        )

    def share_first(plane):
        return pl.multiple_of(direct + plane * shared, 16)

    chunks = [(s, q) for s in range(1, groups) for q in range(4)]

    def grads_shared(e):
        s, q = chunks[e]
        return grads_over(s, q, share_first(mp), shared, gs_s.at[e], gs_r.at[e])

    def grads_direct(e):
        s, q = chunks[e]
        return grads_over(s, q, 0, direct, gd_s.at[e], gd_r.at[e])

    def share(e, plane):
        s, q = chunks[e]
        return peer_g.at[s - 1, pl.ds(share_first(plane), shared), pl.ds(q * depth, depth)]

    def relay_up(e, r):
        ref = share(e, mp - r)
        return remote(ref, ref, zr_s.at[e, r], zr_r.at[e, r + 1], at_mp(mp + 1))

    def relay_down(e, r):
        ref = share(e, mp + r)
        return remote(ref, ref, zl_s.at[e, r], zl_r.at[e, r + 1], at_mp(mp - 1))

    def from_below(e, r):
        ref = share(e, mp - r)
        return remote(ref, ref, zr_s.at[e, r], zr_r.at[e, r], at_mp(mp - 1))

    def from_above(e, r):
        ref = share(e, mp + r)
        return remote(ref, ref, zl_s.at[e, r], zl_r.at[e, r], at_mp(mp + 1))

    tables = ((q_left, left), (q_right, right))
    mine = group * 4 + place
    theirs = group * 4 + places[2]

    def query_across(k):
        source, table = tables[k]
        return remote(source, table.at[rows_of(mine), :], qx_s.at[k], qx_r.at[k], across)

    def query_arrived_across(k):
        source, table = tables[k]
        return remote(source, table.at[rows_of(theirs), :], qx_s.at[k], qx_r.at[k], across)

    def query_over(s, j, k):
        source, table = tables[k]
        slot = ((s - 1) * 2 + j) * 2 + k
        rows = table.at[rows_of((mine, theirs)[j]), :]
        return remote(source if j == 0 else rows, rows, qy_s.at[slot], qy_r.at[slot], peer(s))

    def query_arrived_over(s, j, k):
        table = tables[k][1]
        slot = ((s - 1) * 2 + j) * 2 + k
        origin = group_at(groups - s) * 4 + (place, places[2])[j]
        rows = table.at[rows_of(origin), :]
        return remote(rows, rows, qy_s.at[slot], qy_r.at[slot], peer(groups - s))

    def query_partner(s, j, k):
        source, table = tables[k]
        slot = (s * 2 + j) * 2 + k
        origin = group_at(groups - s) * 4 + (place, places[2])[j]
        rows = table.at[rows_of(origin), :]
        first = source if s == 0 and j == 0 else rows
        return remote(first, rows, qd_s.at[slot], qd_r.at[slot], partner)

    def query_arrived_partner(s, j, k):
        table = tables[k][1]
        slot = (s * 2 + j) * 2 + k
        origin = group_at(groups - s) * 4 + (places[1], places[3])[j]
        rows = table.at[rows_of(origin), :]
        return remote(rows, rows, qd_s.at[slot], qd_r.at[slot], partner)

    for p in range(2):
        go(basis_across(p, size_of(p)))
    for e in range(len(chunks)):
        go(grads_shared(e))
    for k in range(2):
        go(query_across(k))
    for p in range(2, pieces):
        go(basis_across(p, size_of(p)))
    go(basis_partner)
    for k in range(2):
        go(query_partner(0, 0, k))
    for e in range(len(chunks)):
        go(grads_direct(e))
    for s in range(1, groups):
        for k in range(2):
            go(query_over(s, 0, k))

    k_chunks = acts.shape[1] // act_buf.shape[2]
    k_size = act_buf.shape[2]

    def load_chunk(i):
        slot = i % 2
        return (
            pltpu.make_async_copy(
                acts.at[:, pl.ds(i * k_size, k_size)], act_buf.at[slot], chunk_sem.at[slot, 0]
            ),
            pltpu.make_async_copy(
                in_basis.at[pl.ds(i * k_size, k_size), :], inb_buf.at[slot], chunk_sem.at[slot, 1]
            ),
        )

    for copy in load_chunk(0):
        copy.start()
    loads = [pltpu.make_async_copy(out_basis, basis.at[pl.ds(0, depth), :], load_sem.at[0])]
    for q in range(4):
        start = (group * 4 + places[q]) * depth
        loads.append(
            pltpu.make_async_copy(
                grads.at[:, pl.ds(pl.multiple_of(start, 128), depth)],
                own_g.at[:, pl.ds(q * depth, depth)],
                load_sem.at[1 + q],
            )
        )
    for k in range(2):
        loads.append(
            pltpu.make_async_copy(tables[k][0], tables[k][1].at[rows_of(mine), :], load_sem.at[5 + k])
        )
    for copy in loads:
        copy.start()

    def load_eig(p, size):
        slot = p % 2 if isinstance(p, int) else lax.rem(p, 2)
        return pltpu.make_async_copy(
            eigen.at[:, piece(p, size)], eig.at[slot, :, pl.ds(0, size)], eig_sem.at[slot]
        )

    load_eig(0, size_of(0)).start()

    for i in range(k_chunks):
        if i + 1 < k_chunks:
            for copy in load_chunk(i + 1):
                copy.start()
        for copy in load_chunk(i):
            copy.wait()
        term = jnp.dot(act_buf[i % 2], inb_buf[i % 2], preferred_element_type=jnp.float32)
        if i == 0:
            acc[:, :in_cols] = term
        else:
            acc[:, :in_cols] += term
    rin_rows = pl.ds(pl.multiple_of(mp * in_cols, in_cols), in_cols)
    rin[rin_rows, :] = jnp.transpose(acc[:, :in_cols]).astype(jnp.bfloat16)

    live = length[0, 0]
    active_row = lax.broadcasted_iota(jnp.int32, (1, tokens), 1) < live
    active_col = lax.broadcasted_iota(jnp.int32, (tokens, 1), 0) < live
    columns = jnp.broadcast_to(ids[...], (tokens, tokens))
    same = (jnp.transpose(columns) == columns) & active_row
    repeats = jnp.sum(jnp.where(same, 1.0, 0.0), axis=1, keepdims=True)
    weight[...] = jnp.where(active_col, 1.0 / jnp.maximum(repeats, 1.0), 0.0)
    sums[...] = jnp.zeros_like(sums)

    def up_if(r):
        return (mp >= r) & (mp < n_mp - 1)

    def down_if(r):
        return (mp + r <= n_mp - 1) & (mp > 0)

    for step in range(len(chunks) + n_mp - 1):
        if step < len(chunks):
            grads_shared(step).wait_recv()
        for r in range(n_mp):
            e = step - r
            if not 0 <= e < len(chunks):
                continue

            @pl.when(up_if(r))
            def _():
                if r > 0:
                    from_below(e, r).wait_recv()
                relay_up(e, r).start()

            @pl.when(down_if(r))
            def _():
                if r > 0:
                    from_above(e, r).wait_recv()
                relay_down(e, r).start()

    def rin_over(m):
        ref = rin.at[rin_rows, :]
        return remote(ref, ref, rz_s.at[m], rz_r.at[m], at_mp(lax.rem(mp + m, n_mp)))

    def rin_arrived(m):
        source = lax.rem(mp + n_mp - m, n_mp)
        ref = rin.at[pl.ds(pl.multiple_of(source * in_cols, in_cols), in_cols), :]
        return remote(ref, ref, rz_s.at[m], rz_r.at[m], at_mp(source))

    def relay_queries():
        for k in range(2):
            query_arrived_across(k).wait_recv()
            for s in range(1, groups):
                query_over(s, 1, k).start()
            query_partner(0, 1, k).start()

    def send_rin():
        for m in range(1, n_mp):
            rin_over(m).start()

    for copy in loads:
        copy.wait()
    basis_partner.wait_recv()

    def part_over(s, p, size):
        return remote(
            part_out.at[s - 1, :, piece(p, size)],
            part_in.at[s - 1, :, piece(p, size)],
            ss_s.at[s - 1, p],
            ss_r.at[s - 1, p],
            peer(groups - s),
        )

    def term(rows, p, size, first, count):
        k = pl.ds(first * depth, count * depth)
        return jnp.dot(rows[:, k], basis[k, piece(p, size)], preferred_element_type=jnp.float32)

    def room(j, size):
        return pl.ds(j * width, size)

    def own(p, size):
        mine = room(0, size)
        acc[:, mine] = term(own_g, p, size, 0, 2)
        basis_across(p, size).wait_recv()
        basis_forward(p, size).start()
        acc[:, mine] += term(own_g, p, size, 2, 1)
        basis_forward(p, size).wait_recv()
        total = acc[:, mine] + term(own_g, p, size, 3, 1)
        own_out[:, piece(p, size)] = total.astype(jnp.bfloat16)

    def parts(p, size):
        for j in range(groups - 1):
            total = term(peer_g.at[j], p, size, 0, 4)
            part_out[j, :, piece(p, size)] = total.astype(jnp.bfloat16)
            part_over(j + 1, p, size).start()

    rows_from = [peer_g.at[s - 1] for s in range(1, groups)] + [own_g]

    def rotate(p, size):
        for j, rows in enumerate(rows_from):
            acc[:, room(j, size)] = term(rows, p, size, 0, 2)
        basis_across(p, size).wait_recv()
        basis_forward(p, size).start()
        for j, rows in enumerate(rows_from):
            acc[:, room(j, size)] += term(rows, p, size, 2, 1)
        basis_forward(p, size).wait_recv()
        for j, rows in enumerate(rows_from):
            total = acc[:, room(j, size)] + term(rows, p, size, 3, 1)
            if j < groups - 1:
                part_out[j, :, piece(p, size)] = total.astype(jnp.bfloat16)
                part_over(j + 1, p, size).start()
            else:
                own_out[:, piece(p, size)] = total.astype(jnp.bfloat16)

    def factors_arrive():
        for m in range(1, n_mp):
            rin_arrived(m).wait_recv()
        for s in range(1, groups):
            for j in range(2):
                for k in range(2):
                    query_arrived_over(s, j, k).wait_recv()
                    query_partner(s, j, k).start()
        for s in range(groups):
            for j in range(2):
                for k in range(2):
                    query_arrived_partner(s, j, k).wait_recv()

    def score(p, size):
        static = isinstance(p, int)
        load_eig(p, size).wait()
        if static:
            if p + 1 < pieces:
                load_eig(p + 1, size_of(p + 1)).start()
        else:

            @pl.when(p + 1 < wide)
            def _():
                load_eig(p + 1, size).start()

            @pl.when(p + 1 == wide)
            def _():
                load_eig(wide, ends[0]).start()

        total = own_out[:, piece(p, size)].astype(jnp.float32)
        for s in range(1, groups):
            part_over(s, p, size).wait_recv()
            total = total + part_in[s - 1, :, piece(p, size)].astype(jnp.float32)
        rotated = total.astype(jnp.bfloat16).astype(jnp.float32)
        scaled = (weight[...] * rotated).astype(jnp.bfloat16)
        slot = p % 2 if static else lax.rem(p, 2)
        block = 512
        for i in range(0, kin, block):
            rows = pl.ds(i, block)
            gradient = jnp.dot(rin[rows, :], scaled, preferred_element_type=jnp.float32)
            denominator = eig[slot, rows, pl.ds(0, size)].astype(jnp.float32) + damping
            cond[rows, pl.ds(0, size)] = (gradient / denominator).astype(jnp.bfloat16)
        for i in range(0, left.shape[0], block):
            rows = pl.ds(i, block)
            mixture = jnp.dot(
                left[rows, :], cond[:, pl.ds(0, size)], preferred_element_type=jnp.float32
            )
            weighted = mixture * right[rows, piece(p, size)].astype(jnp.float32)
            folded = weighted[:, :128]
            for c in range(128, size, 128):
                folded = folded + weighted[:, c : c + 128]
            sums[rows, :] += folded

    def first(p, carry):
        @pl.when(p == early - 1)
        def _():
            relay_queries()
            send_rin()

        own(p, width)
        return carry

    lax.fori_loop(0, early, first, 0)

    for e in range(len(chunks)):
        grads_direct(e).wait_recv()
        for r in range(1, n_mp):

            @pl.when((mp >= r) & (mp == n_mp - 1))
            def _():
                from_below(e, r).wait_recv()

            @pl.when((mp + r <= n_mp - 1) & (mp == 0))
            def _():
                from_above(e, r).wait_recv()

    def step(p, carry):
        @pl.when(p < early)
        def _():
            parts(p, width)

        @pl.when((p >= early) & (p < wide))
        def _():
            rotate(p, width)

        for t, size in enumerate(ends):

            @pl.when(p == wide + t)
            def _():
                rotate(wide + t, size)

        @pl.when(p == LAG)
        def _():
            factors_arrive()

        @pl.when(p >= LAG)
        def _():
            score(p - LAG, width)

        return carry

    lax.fori_loop(0, wide + LAG, step, 0)
    for t, size in enumerate(ends):
        score(wide + t, size)

    queries, rank = out.shape[0], left.shape[0] // out.shape[0]
    gathered[0] = jnp.sum(sums[...].reshape(queries, rank, 128), axis=1)

    def score_over(m):
        return remote(
            gathered.at[0],
            gathered.at[m],
            sc_s.at[m],
            sc_r.at[m],
            at_mp(lax.rem(mp + m, n_mp)),
        )

    for m in range(1, n_mp):
        go(score_over(m))
    total = gathered[0]
    for m in range(1, n_mp):
        score_over(m).wait_recv()
        total = total + gathered[m]
    out[...] = total

    for copy in sends:
        copy.wait_send()
    for m in range(1, n_mp):
        rin_over(m).wait_send()
    for k in range(2):
        for s in range(1, groups):
            query_over(s, 1, k).wait_send()
        query_partner(0, 1, k).wait_send()
    for s in range(1, groups):
        for j in range(2):
            for k in range(2):
                query_partner(s, j, k).wait_send()

    def sent(p, size):
        basis_forward(p, size).wait_send()
        for s in range(1, groups):
            part_over(s, p, size).wait_send()

    for p in range(pieces):
        sent(p, size_of(p))
    for e in range(len(chunks)):
        for r in range(n_mp):

            @pl.when(up_if(r))
            def _():
                relay_up(e, r).wait_send()

            @pl.when(down_if(r))
            def _():
                relay_down(e, r).wait_send()


def per_device(
    n_dp,
    n_mp,
    doc_ids,
    doc_lengths,
    activations,
    out_grads,
    input_basis,
    output_basis,
    eigenvalues,
    query_left,
    query_right,
):
    groups = n_dp // 4
    tokens = out_grads.shape[0]
    depth, cols = output_basis.shape
    kin = eigenvalues.shape[0]
    in_cols = input_basis.shape[1]
    per_block, rank = query_left.shape[:2]
    q_rows = per_block * rank
    queries = n_dp * per_block
    width, wide, ends = piece_plan(cols)
    pieces = wide + len(ends)
    chunks = (groups - 1) * 4
    k_size = 512
    bf16, f32 = jnp.bfloat16, jnp.float32

    def pair(*shape):
        return [pltpu.SemaphoreType.DMA(shape), pltpu.SemaphoreType.DMA(shape)]

    vmem = pl.BlockSpec(memory_space=pltpu.VMEM)
    hbm = pl.BlockSpec(memory_space=pl.ANY)
    summed = pl.pallas_call(
        functools.partial(kernel, n_dp, n_mp),
        out_shape=jax.ShapeDtypeStruct((queries, 128), f32),
        in_specs=[vmem, pl.BlockSpec(memory_space=pltpu.SMEM)] + [hbm] * 7,
        out_specs=vmem,
        scratch_shapes=[
            pltpu.VMEM((4 * depth, cols), bf16),
            pltpu.VMEM((tokens, 4 * depth), bf16),
            pltpu.VMEM((groups - 1, tokens, 4 * depth), bf16),
            pltpu.VMEM((kin, tokens), bf16),
            pltpu.VMEM((n_dp * q_rows, kin), bf16),
            pltpu.VMEM((n_dp * q_rows, cols), bf16),
            pltpu.VMEM((2, kin, width), bf16),
            pltpu.VMEM((groups - 1, tokens, cols), bf16),
            pltpu.VMEM((groups - 1, tokens, cols), bf16),
            pltpu.VMEM((tokens, cols), bf16),
            pltpu.VMEM((2, tokens, k_size), bf16),
            pltpu.VMEM((2, k_size, in_cols), bf16),
            pltpu.VMEM((tokens, max(in_cols, groups * width)), f32),
            pltpu.VMEM((kin, width), bf16),
            pltpu.VMEM((tokens, 1), f32),
            pltpu.VMEM((n_dp * q_rows, 128), f32),
            pltpu.VMEM((n_mp, queries, 128), f32),
            pltpu.SemaphoreType.DMA((7,)),
            pltpu.SemaphoreType.DMA((2, 2)),
            pltpu.SemaphoreType.DMA((2,)),
            *pair(pieces),
            *pair(1),
            *pair(pieces),
            *pair(chunks),
            *pair(chunks),
            *pair(chunks, n_mp + 1),
            *pair(chunks, n_mp + 1),
            *pair(n_mp),
            *pair(2),
            *pair((groups - 1) * 4),
            *pair(groups * 4),
            *pair(groups - 1, pieces),
            *pair(n_mp),
        ],
        compiler_params=pltpu.CompilerParams(
            collective_id=0, has_side_effects=True, vmem_limit_bytes=67043328
        ),
    )(
        doc_ids,
        doc_lengths.reshape(1, 1),
        activations,
        out_grads,
        input_basis,
        output_basis,
        eigenvalues,
        query_left.reshape(q_rows, kin),
        query_right.reshape(q_rows, cols),
    )
    return jnp.sum(summed, axis=1).reshape(1, queries)


def solution(mesh):
    return jax.shard_map(
        functools.partial(per_device, mesh.shape["dp"], mesh.shape["mp"]),
        mesh=mesh,
        in_specs=(
            P("dp", None),
            P("dp"),
            P("dp", None),
            P("dp", None),
            P(None, "mp"),
            P("dp", "mp"),
            P(None, "mp"),
            P("dp", None, None),
            P("dp", None, "mp"),
        ),
        out_specs=P("dp", None),
        check_vma=False,
    )
```

```python
import functools

import jax
import jax.numpy as jnp
from jax import lax
from jax.experimental import pallas as pl
from jax.experimental.pallas import tpu as pltpu
from jax.sharding import PartitionSpec as P

damping = 0.5
EARLY = 3
SHARED = (8, 8, 10, 10)


def piece_plan(columns):
    width = 256 if columns % 256 == 0 else 128
    return width, columns // width - 1, [128] * (width // 128)


def kernel(
    n_dp,
    n_mp,
    ids,
    length,
    acts,
    grads,
    in_basis,
    out_basis,
    eigen,
    q_left,
    q_right,
    out,
    basis,
    own_g,
    peer_g,
    rin,
    left,
    right,
    eig,
    part_out,
    part_in,
    own_out,
    act_buf,
    inb_buf,
    acc,
    acc_end,
    cond,
    weight,
    sums,
    gathered,
    load_sem,
    chunk_sem,
    eig_sem,
    bx_s,
    bx_r,
    bd_s,
    bd_r,
    bf_s,
    bf_r,
    gs_s,
    gs_r,
    gd_s,
    gd_r,
    zr_s,
    zr_r,
    zl_s,
    zl_r,
    qx_s,
    qx_r,
    qy_s,
    qy_r,
    qd_s,
    qd_r,
    lx_s,
    lx_r,
    ly_s,
    ly_r,
    iu_s,
    iu_r,
    id_s,
    id_r,
    ld_s,
    ld_r,
    ss_s,
    ss_r,
    sc_s,
    sc_r,
):
    groups = n_dp // 4
    dp, mp = lax.axis_index("dp"), lax.axis_index("mp")
    group, place = lax.div(dp, 4), lax.rem(dp, 4)
    places = (place, place + 1 - 2 * lax.rem(place, 2), lax.rem(place + 2, 4), 3 - place)

    tokens = grads.shape[0]
    depth, cols = out_basis.shape
    width, wide, ends = piece_plan(cols)
    pieces = wide + len(ends)
    early = min(EARLY, wide)
    in_cols = in_basis.shape[1]
    kin = rin.shape[0]
    q_rows = q_right.shape[0]
    slice_rows = q_left.shape[1]
    halves = n_dp // 2
    shared = [tokens * parts // 16 // n_mp // 16 * 16 for parts in SHARED]
    direct = [tokens - rows * n_mp for rows in shared]

    def at_dp(index):
        return (index, mp)

    def at_mp(index):
        return (dp, index)

    partner = at_dp(group * 4 + places[1])
    across = at_dp(group * 4 + places[2])

    def group_at(s):
        return lax.rem(group + s, groups)

    def peer(s):
        return at_dp(group_at(s) * 4 + place)

    def remote(src, dst, send, recv, device):
        return pltpu.make_async_remote_copy(
            src_ref=src,
            dst_ref=dst,
            send_sem=send,
            recv_sem=recv,
            device_id=device,
            device_id_type=pl.DeviceIdType.MESH,
        )

    barrier = pltpu.get_barrier_semaphore()
    friends = [partner, across]
    friends += [peer(s) for s in range(1, groups)]
    friends += [at_mp(lax.rem(mp + m, n_mp)) for m in range(1, n_mp)]
    for friend in friends:
        pl.semaphore_signal(barrier, inc=1, device_id=friend, device_id_type=pl.DeviceIdType.MESH)
    pl.semaphore_wait(barrier, len(friends))

    sends = []

    def go(copy):
        copy.start()
        sends.append(copy)

    def piece(p, size):
        if size == width and not isinstance(p, int):
            return pl.ds(pl.multiple_of(p * width, width), width)
        return pl.ds(p * width if p < wide else wide * width + (p - wide) * 128, size)

    def size_of(p):
        return width if p < wide else ends[p - wide]

    def basis_across(p, size):
        return remote(
            out_basis.at[:, piece(p, size)],
            basis.at[pl.ds(2 * depth, depth), piece(p, size)],
            bx_s.at[p],
            bx_r.at[p],
            across,
        )

    def basis_forward(p, size):
        return remote(
            basis.at[pl.ds(2 * depth, depth), piece(p, size)],
            basis.at[pl.ds(3 * depth, depth), piece(p, size)],
            bf_s.at[p],
            bf_r.at[p],
            partner,
        )

    basis_partner = remote(
        out_basis, basis.at[pl.ds(depth, depth), :], bd_s.at[0], bd_r.at[0], partner
    )

    def grads_over(s, q, rows, send, recv):
        start = (group_at(s) * 4 + places[q]) * depth
        return remote(
            grads.at[rows, pl.ds(pl.multiple_of(start, 128), depth)],
            peer_g.at[s - 1, rows, pl.ds(q * depth, depth)],
            send,
            recv,
            peer(s),
        )

    def share_rows(q, plane):
        return pl.ds(pl.multiple_of(direct[q] + plane * shared[q], 16), shared[q])

    chunks = [(s, q) for s in range(1, groups) for q in range(4)]

    def grads_shared(e):
        s, q = chunks[e]
        return grads_over(s, q, share_rows(q, mp), gs_s.at[e], gs_r.at[e])

    def grads_direct(e):
        s, q = chunks[e]
        return grads_over(s, q, pl.ds(0, direct[q]), gd_s.at[e], gd_r.at[e])

    def share(e, plane):
        s, q = chunks[e]
        return peer_g.at[s - 1, share_rows(q, plane), pl.ds(q * depth, depth)]

    def relay_up(e, r):
        ref = share(e, mp - r)
        return remote(ref, ref, zr_s.at[e, r], zr_r.at[e, r + 1], at_mp(mp + 1))

    def relay_down(e, r):
        ref = share(e, mp + r)
        return remote(ref, ref, zl_s.at[e, r], zl_r.at[e, r + 1], at_mp(mp - 1))

    def from_below(e, r):
        ref = share(e, mp - r)
        return remote(ref, ref, zr_s.at[e, r], zr_r.at[e, r], at_mp(mp - 1))

    def from_above(e, r):
        ref = share(e, mp + r)
        return remote(ref, ref, zl_s.at[e, r], zl_r.at[e, r], at_mp(mp + 1))

    core = lax.rem(place, 2)

    def half(s, j):
        chip = lax.div(place, 2)
        return group_at(groups - s) * 2 + (chip if j == 0 else 1 - chip)

    def right_across():
        return remote(q_right, right.at[core, half(0, 0)], qx_s.at[0], qx_r.at[0], across)

    def right_arrived_across():
        return remote(q_right, right.at[core, half(0, 1)], qx_s.at[0], qx_r.at[0], across)

    def right_over(s, j):
        rows = right.at[core, half(0, j)]
        slot = (s - 1) * 2 + j
        return remote(q_right if j == 0 else rows, rows, qy_s.at[slot], qy_r.at[slot], peer(s))

    def right_arrived_over(s, j):
        rows = right.at[core, half(s, j)]
        slot = (s - 1) * 2 + j
        return remote(rows, rows, qy_s.at[slot], qy_r.at[slot], peer(groups - s))

    def right_partner(s, j):
        rows = right.at[core, half(s, j)]
        slot = s * 2 + j
        first = q_right if s == 0 and j == 0 else rows
        return remote(first, rows, qd_s.at[slot], qd_r.at[slot], partner)

    def right_arrived_partner(s, j):
        rows = right.at[1 - core, half(s, j)]
        slot = s * 2 + j
        return remote(rows, rows, qd_s.at[slot], qd_r.at[slot], partner)

    def left_across():
        return remote(
            q_left.at[mp], left.at[mp, core, half(0, 0)], lx_s.at[0], lx_r.at[0], across
        )

    def left_arrived_across():
        return remote(
            q_left.at[mp], left.at[mp, core, half(0, 1)], lx_s.at[0], lx_r.at[0], across
        )

    def left_over(s, j):
        rows = left.at[mp, core, half(0, j)]
        slot = (s - 1) * 2 + j
        return remote(
            q_left.at[mp] if j == 0 else rows, rows, ly_s.at[slot], ly_r.at[slot], peer(s)
        )

    def left_arrived_over(s, j):
        rows = left.at[mp, core, half(s, j)]
        slot = (s - 1) * 2 + j
        return remote(rows, rows, ly_s.at[slot], ly_r.at[slot], peer(groups - s))

    def left_partner(plane):
        rows = left.at[plane, core]
        return remote(rows, rows, ld_s.at[plane], ld_r.at[plane], partner)

    def left_arrived_partner(plane):
        rows = left.at[plane, 1 - core]
        return remote(rows, rows, ld_s.at[plane], ld_r.at[plane], partner)

    foreign = [(s, j) for s in range(groups) for j in range(2) if s + j > 0]
    items = 1 + len(foreign)

    def item(i, plane):
        if i == 0:
            return rin.at[pl.ds(pl.multiple_of(plane * in_cols, in_cols), in_cols), :]
        s, j = foreign[i - 1]
        return left.at[plane, core, half(s, j)]

    def item_up(i, r):
        ref = item(i, mp - r)
        return remote(ref, ref, iu_s.at[i, r], iu_r.at[i, r + 1], at_mp(mp + 1))

    def item_down(i, r):
        ref = item(i, mp + r)
        return remote(ref, ref, id_s.at[i, r], id_r.at[i, r + 1], at_mp(mp - 1))

    def item_below(i, r):
        ref = item(i, mp - r)
        return remote(ref, ref, iu_s.at[i, r], iu_r.at[i, r], at_mp(mp - 1))

    def item_above(i, r):
        ref = item(i, mp + r)
        return remote(ref, ref, id_s.at[i, r], id_r.at[i, r], at_mp(mp + 1))

    go(left_across())
    for e in range(len(chunks)):
        go(grads_shared(e))
    for s in range(1, groups):
        go(left_over(s, 0))
    for p in range(2):
        go(basis_across(p, size_of(p)))
    go(right_across())
    for p in range(2, pieces):
        go(basis_across(p, size_of(p)))
    go(basis_partner)
    go(right_partner(0, 0))

    k_chunks = acts.shape[1] // act_buf.shape[2]
    k_size = act_buf.shape[2]

    def load_chunk(i):
        slot = i % 2
        return (
            pltpu.make_async_copy(
                acts.at[:, pl.ds(i * k_size, k_size)], act_buf.at[slot], chunk_sem.at[slot, 0]
            ),
            pltpu.make_async_copy(
                in_basis.at[pl.ds(i * k_size, k_size), :], inb_buf.at[slot], chunk_sem.at[slot, 1]
            ),
        )

    for copy in load_chunk(0):
        copy.start()
    loads = [pltpu.make_async_copy(out_basis, basis.at[pl.ds(0, depth), :], load_sem.at[0])]
    for q in range(4):
        start = (group * 4 + places[q]) * depth
        loads.append(
            pltpu.make_async_copy(
                grads.at[:, pl.ds(pl.multiple_of(start, 128), depth)],
                own_g.at[:, pl.ds(q * depth, depth)],
                load_sem.at[1 + q],
            )
        )
    loads.append(pltpu.make_async_copy(q_left, left.at[:, core, half(0, 0)], load_sem.at[5]))
    loads.append(pltpu.make_async_copy(q_right, right.at[core, half(0, 0)], load_sem.at[6]))
    for copy in loads:
        copy.start()

    def load_eig(p):
        slot = p % 2 if isinstance(p, int) else lax.rem(p, 2)
        return pltpu.make_async_copy(eigen.at[:, piece(p, width)], eig.at[slot], eig_sem.at[slot])

    load_eig(0).start()

    for i in range(k_chunks):
        if i + 1 < k_chunks:
            for copy in load_chunk(i + 1):
                copy.start()
        for copy in load_chunk(i):
            copy.wait()
        term = jnp.dot(act_buf[i % 2], inb_buf[i % 2], preferred_element_type=jnp.float32)
        if i == 0:
            acc[:, :in_cols] = term
        else:
            acc[:, :in_cols] += term
    rin_rows = pl.ds(pl.multiple_of(mp * in_cols, in_cols), in_cols)
    rin[rin_rows, :] = jnp.transpose(acc[:, :in_cols]).astype(jnp.bfloat16)

    def weigh():
        live = length[0, 0]
        active_row = lax.broadcasted_iota(jnp.int32, (1, tokens), 1) < live
        active_col = lax.broadcasted_iota(jnp.int32, (tokens, 1), 0) < live
        columns = jnp.broadcast_to(ids[...], (tokens, tokens))
        same = (jnp.transpose(columns) == columns) & active_row
        repeats = jnp.sum(jnp.where(same, 1.0, 0.0), axis=1, keepdims=True)
        weight[...] = jnp.where(active_col, 1.0 / jnp.maximum(repeats, 1.0), 0.0)
        sums[...] = jnp.zeros_like(sums)

    left_arrived_across().wait_recv()
    for s in range(1, groups):
        go(left_over(s, 1))
    for e in range(len(chunks)):
        go(grads_direct(e))
    for s in range(1, groups):
        go(right_over(s, 0))

    def up_if(r):
        return (mp >= r) & (mp < n_mp - 1)

    def down_if(r):
        return (mp + r <= n_mp - 1) & (mp > 0)

    for step in range(len(chunks) + n_mp - 1):
        if step < len(chunks):
            grads_shared(step).wait_recv()
        for r in range(n_mp):
            e = step - r
            if not 0 <= e < len(chunks):
                continue

            @pl.when(up_if(r))
            def _():
                if r > 0:
                    from_below(e, r).wait_recv()
                relay_up(e, r).start()

            @pl.when(down_if(r))
            def _():
                if r > 0:
                    from_above(e, r).wait_recv()
                relay_down(e, r).start()

        if step == 0:
            weigh()

    def relay_items(r):
        @pl.when(up_if(r))
        def _():
            for i in range(items):
                if r > 0:
                    item_below(i, r).wait_recv()
                item_up(i, r).start()

        @pl.when(down_if(r))
        def _():
            for i in range(items):
                if r > 0:
                    item_above(i, r).wait_recv()
                item_down(i, r).start()

    for s in range(1, groups):
        for j in range(2):
            left_arrived_over(s, j).wait_recv()
    relay_items(0)

    def relay_right():
        right_arrived_across().wait_recv()
        for s in range(1, groups):
            right_over(s, 1).start()
        right_partner(0, 1).start()

    for copy in loads:
        copy.wait()
    basis_partner.wait_recv()

    def part_over(s, p, size):
        return remote(
            part_out.at[s - 1, :, piece(p, size)],
            part_in.at[s - 1, :, piece(p, size)],
            ss_s.at[s - 1, p],
            ss_r.at[s - 1, p],
            peer(groups - s),
        )

    def term(rows, p, size, first, count):
        k = pl.ds(first * depth, count * depth)
        return jnp.dot(rows[:, k], basis[k, piece(p, size)], preferred_element_type=jnp.float32)

    def room(j, size):
        return pl.ds(j * width, size)

    def own(p, size):
        mine = room(0, size)
        basis_across(p, size).wait_recv()
        basis_forward(p, size).start()
        acc[:, mine] = term(own_g, p, size, 0, 3)
        basis_forward(p, size).wait_recv()
        total = acc[:, mine] + term(own_g, p, size, 3, 1)
        own_out[:, piece(p, size)] = total.astype(jnp.bfloat16)

    def parts(p, size):
        for j in range(groups - 1):
            total = term(peer_g.at[j], p, size, 0, 4)
            part_out[j, :, piece(p, size)] = total.astype(jnp.bfloat16)
            part_over(j + 1, p, size).start()

    rows_from = [peer_g.at[s - 1] for s in range(1, groups)] + [own_g]

    def rotate(p, size):
        basis_across(p, size).wait_recv()
        basis_forward(p, size).start()
        for j, rows in enumerate(rows_from):
            acc[:, room(j, size)] = term(rows, p, size, 0, 3)
        basis_forward(p, size).wait_recv()
        for j, rows in enumerate(rows_from):
            total = acc[:, room(j, size)] + term(rows, p, size, 3, 1)
            finish(j, p, size, total)

    def finish(j, p, size, total):
        if j < groups - 1:
            part_out[j, :, piece(p, size)] = total.astype(jnp.bfloat16)
            part_over(j + 1, p, size).start()
        else:
            own_out[:, piece(p, size)] = total.astype(jnp.bfloat16)

    def prepare():
        for j, rows in enumerate(rows_from):
            acc_end[:, room(j, width)] = term(rows, wide, width, 0, 2)

    def rotate_end(t):
        p, size = wide + t, ends[t]
        basis_across(p, size).wait_recv()
        basis_forward(p, size).start()
        for j, rows in enumerate(rows_from):
            acc_end[:, pl.ds(j * width + t * 128, size)] += term(rows, p, size, 2, 1)
        basis_forward(p, size).wait_recv()
        for j, rows in enumerate(rows_from):
            total = acc_end[:, pl.ds(j * width + t * 128, size)] + term(rows, p, size, 3, 1)
            finish(j, p, size, total)

    def right_arrives():
        for s in range(1, groups):
            for j in range(2):
                right_arrived_over(s, j).wait_recv()
                right_partner(s, j).start()
        left_partner(mp).start()

    def left_arrives(r):
        @pl.when(mp >= r)
        def _():
            @pl.when(mp == n_mp - 1)
            def _():
                for i in range(items):
                    item_below(i, r).wait_recv()

            left_partner(mp - r).start()

        @pl.when(mp + r <= n_mp - 1)
        def _():
            @pl.when(mp == 0)
            def _():
                for i in range(items):
                    item_above(i, r).wait_recv()

            left_partner(mp + r).start()

    def factors_arrive():
        for plane in range(n_mp):
            left_arrived_partner(plane).wait_recv()
        for s in range(groups):
            for j in range(2):
                right_arrived_partner(s, j).wait_recv()

    def score(p, size):
        last = isinstance(p, int)
        load_eig(p).wait()
        if not last:
            load_eig(p + 1).start()
        total = own_out[:, piece(p, size)].astype(jnp.float32)
        for s in range(1, groups):
            if last:
                for t in range(len(ends)):
                    part_over(s, wide + t, ends[t]).wait_recv()
            else:
                part_over(s, p, size).wait_recv()
            total = total + part_in[s - 1, :, piece(p, size)].astype(jnp.float32)
        rotated = total.astype(jnp.bfloat16).astype(jnp.float32)
        scaled = (weight[...] * rotated).astype(jnp.bfloat16)
        slot = p % 2 if last else lax.rem(p, 2)
        block = 512
        for i in range(0, kin, block):
            rows = pl.ds(i, block)
            gradient = jnp.dot(rin[rows, :], scaled, preferred_element_type=jnp.float32)
            denominator = eig[slot, rows, :].astype(jnp.float32) + damping
            cond[rows, :] = (gradient / denominator).astype(jnp.bfloat16)
        for plane in range(n_mp):
            lhs = left[plane].reshape(n_dp * slice_rows, kin)
            factor = right[:, :, pl.ds(plane * slice_rows, slice_rows), piece(p, size)]
            mixture = jnp.dot(lhs, cond[...], preferred_element_type=jnp.float32)
            weighted = mixture * factor.reshape(n_dp * slice_rows, size).astype(jnp.float32)
            folded = weighted[:, :128]
            for c in range(128, size, 128):
                folded = folded + weighted[:, c : c + 128]
            sums[plane] += folded

    def first(p, carry):
        @pl.when(p == early - 1)
        def _():
            relay_right()
            relay_items(1)

        own(p, width)
        return carry

    lax.fori_loop(0, early, first, 0)

    for e in range(len(chunks)):
        grads_direct(e).wait_recv()
        for r in range(1, n_mp):

            @pl.when((mp >= r) & (mp == n_mp - 1))
            def _():
                from_below(e, r).wait_recv()

            @pl.when((mp + r <= n_mp - 1) & (mp == 0))
            def _():
                from_above(e, r).wait_recv()

    for r in range(2, n_mp):
        relay_items(r)

    def scored(p):
        done = jnp.where(p < wide - 1, 0, jnp.where(p == wide + 1, wide, p - wide + 4))
        return jnp.minimum(done, wide)

    def one(i, carry):
        score(i, width)
        return carry

    def step(p, carry):
        @pl.when(p < early)
        def _():
            parts(p, width)

        @pl.when((p >= early) & (p < wide))
        def _():
            rotate(p, width)

        for t in range(len(ends)):

            @pl.when(p == wide + t)
            def _():
                rotate_end(t)

        @pl.when(p == wide - 2)
        def _():
            right_arrives()
            for r in range(1, n_mp - 1):
                left_arrives(r)
            prepare()

        @pl.when(p == wide - 1)
        def _():
            left_arrives(n_mp - 1)
            factors_arrive()

        lax.fori_loop(scored(p - 1), scored(p), one, 0)
        return carry

    lax.fori_loop(0, pieces, step, 0)
    lax.fori_loop(scored(pieces - 1), wide, one, 0)
    score(wide, width)

    per_block = out.shape[0] // n_dp
    rank = q_rows // per_block
    unit = min(rank, slice_rows)
    totals = {}
    for plane in range(n_mp):
        for u in range(slice_rows // unit):
            local = (plane * slice_rows + u * unit) // rank
            block = sums[plane].reshape(n_dp, slice_rows, 128)[:, u * unit : (u + 1) * unit, :]
            found = jnp.sum(block, axis=1)
            totals[local] = totals[local] + found if local in totals else found
    for local, found in totals.items():
        for c in range(2):
            for h in range(halves):
                row = (2 * h + c) * per_block + local
                gathered[0, row : row + 1, :] = found[c * halves + h : c * halves + h + 1, :]

    def score_over(m):
        return remote(
            gathered.at[0],
            gathered.at[m],
            sc_s.at[m],
            sc_r.at[m],
            at_mp(lax.rem(mp + m, n_mp)),
        )

    for m in range(1, n_mp):
        go(score_over(m))
    for copy in sends:
        copy.wait_send()
    for r in range(n_mp):

        @pl.when(up_if(r))
        def _():
            for i in range(items):
                item_up(i, r).wait_send()

        @pl.when(down_if(r))
        def _():
            for i in range(items):
                item_down(i, r).wait_send()

    for s in range(1, groups):
        right_over(s, 1).wait_send()
        for j in range(2):
            right_partner(s, j).wait_send()
    right_partner(0, 1).wait_send()
    for plane in range(n_mp):
        left_partner(plane).wait_send()

    def sent(p, size):
        basis_forward(p, size).wait_send()
        for s in range(1, groups):
            part_over(s, p, size).wait_send()

    for p in range(pieces):
        sent(p, size_of(p))
    for e in range(len(chunks)):
        for r in range(n_mp):

            @pl.when(up_if(r))
            def _():
                relay_up(e, r).wait_send()

            @pl.when(down_if(r))
            def _():
                relay_down(e, r).wait_send()

    total = gathered[0]
    for m in range(1, n_mp):
        score_over(m).wait_recv()
        total = total + gathered[m]
    out[...] = total

def per_device(
    n_dp,
    n_mp,
    doc_ids,
    doc_lengths,
    activations,
    out_grads,
    input_basis,
    output_basis,
    eigenvalues,
    query_left,
    query_right,
):
    groups = n_dp // 4
    tokens = out_grads.shape[0]
    depth, cols = output_basis.shape
    kin = eigenvalues.shape[0]
    in_cols = input_basis.shape[1]
    per_block, rank = query_left.shape[:2]
    q_rows = per_block * rank
    queries = n_dp * per_block
    width, wide, ends = piece_plan(cols)
    pieces = wide + len(ends)
    chunks = (groups - 1) * 4
    k_size = 512
    bf16, f32 = jnp.bfloat16, jnp.float32

    def pair(*shape):
        return [pltpu.SemaphoreType.DMA(shape), pltpu.SemaphoreType.DMA(shape)]

    vmem = pl.BlockSpec(memory_space=pltpu.VMEM)
    hbm = pl.BlockSpec(memory_space=pl.ANY)
    summed = pl.pallas_call(
        functools.partial(kernel, n_dp, n_mp),
        out_shape=jax.ShapeDtypeStruct((queries, 128), f32),
        in_specs=[vmem, pl.BlockSpec(memory_space=pltpu.SMEM)] + [hbm] * 7,
        out_specs=vmem,
        scratch_shapes=[
            pltpu.VMEM((4 * depth, cols), bf16),
            pltpu.VMEM((tokens, 4 * depth), bf16),
            pltpu.VMEM((groups - 1, tokens, 4 * depth), bf16),
            pltpu.VMEM((kin, tokens), bf16),
            pltpu.VMEM((n_mp, 2, n_dp // 2, q_rows // n_mp, kin), bf16),
            pltpu.VMEM((2, n_dp // 2, q_rows, cols), bf16),
            pltpu.VMEM((2, kin, width), bf16),
            pltpu.VMEM((groups - 1, tokens, cols), bf16),
            pltpu.VMEM((groups - 1, tokens, cols), bf16),
            pltpu.VMEM((tokens, cols), bf16),
            pltpu.VMEM((2, tokens, k_size), bf16),
            pltpu.VMEM((2, k_size, in_cols), bf16),
            pltpu.VMEM((tokens, max(in_cols, groups * width)), f32),
            pltpu.VMEM((tokens, groups * width), f32),
            pltpu.VMEM((kin, width), bf16),
            pltpu.VMEM((tokens, 1), f32),
            pltpu.VMEM((n_mp, n_dp * q_rows // n_mp, 128), f32),
            pltpu.VMEM((n_mp, queries, 128), f32),
            pltpu.SemaphoreType.DMA((7,)),
            pltpu.SemaphoreType.DMA((2, 2)),
            pltpu.SemaphoreType.DMA((2,)),
            *pair(pieces),
            *pair(1),
            *pair(pieces),
            *pair(chunks),
            *pair(chunks),
            *pair(chunks, n_mp + 1),
            *pair(chunks, n_mp + 1),
            *pair(1),
            *pair((groups - 1) * 2),
            *pair(groups * 2),
            *pair(1),
            *pair((groups - 1) * 2),
            *pair(groups * 2, n_mp + 1),
            *pair(groups * 2, n_mp + 1),
            *pair(n_mp),
            *pair(groups - 1, pieces),
            *pair(n_mp),
        ],
        compiler_params=pltpu.CompilerParams(
            collective_id=0, has_side_effects=True, vmem_limit_bytes=67043328
        ),
    )(
        doc_ids,
        doc_lengths.reshape(1, 1),
        activations,
        out_grads,
        input_basis,
        output_basis,
        eigenvalues,
        query_left.reshape(n_mp, q_rows // n_mp, kin),
        query_right.reshape(q_rows, cols),
    )
    return jnp.sum(summed, axis=1).reshape(1, queries)


def solution(mesh):
    return jax.shard_map(
        functools.partial(per_device, mesh.shape["dp"], mesh.shape["mp"]),
        mesh=mesh,
        in_specs=(
            P("dp", None),
            P("dp"),
            P("dp", None),
            P("dp", None),
            P(None, "mp"),
            P("dp", "mp"),
            P(None, "mp"),
            P("dp", None, None),
            P("dp", None, "mp"),
        ),
        out_specs=P("dp", None),
        check_vma=False,
    )
```

```python
import functools

import jax
import jax.numpy as jnp
from jax import lax
from jax.experimental import pallas as pl
from jax.experimental.pallas import tpu as pltpu
from jax.sharding import PartitionSpec as P

damping = 0.5
EARLY = 3
SHARED = (8, 8, 10, 10)


def piece_plan(columns):
    width = 256 if columns % 256 == 0 else 128
    return width, columns // width - 1, [128] * (width // 128)


def kernel(
    n_dp,
    n_mp,
    ids,
    length,
    acts,
    grads,
    in_basis,
    out_basis,
    eigen,
    q_left,
    q_right,
    out,
    basis,
    own_g,
    peer_g,
    rin,
    left,
    right,
    eig,
    part_out,
    part_in,
    own_out,
    act_buf,
    inb_buf,
    acc,
    acc_end,
    cond,
    weight,
    sums,
    gathered,
    load_sem,
    chunk_sem,
    eig_sem,
    bx_s,
    bx_r,
    bd_s,
    bd_r,
    bf_s,
    bf_r,
    gs_s,
    gs_r,
    gd_s,
    gd_r,
    zr_s,
    zr_r,
    zl_s,
    zl_r,
    qx_s,
    qx_r,
    qy_s,
    qy_r,
    qd_s,
    qd_r,
    lx_s,
    lx_r,
    ly_s,
    ly_r,
    iu_s,
    iu_r,
    id_s,
    id_r,
    ld_s,
    ld_r,
    ss_s,
    ss_r,
    sc_s,
    sc_r,
):
    groups = n_dp // 4
    dp, mp = lax.axis_index("dp"), lax.axis_index("mp")
    group, place = lax.div(dp, 4), lax.rem(dp, 4)
    places = (place, place + 1 - 2 * lax.rem(place, 2), lax.rem(place + 2, 4), 3 - place)

    tokens = grads.shape[0]
    depth, cols = out_basis.shape
    width, wide, ends = piece_plan(cols)
    pieces = wide + len(ends)
    early = min(EARLY, wide)
    in_cols = in_basis.shape[1]
    kin = rin.shape[0]
    q_rows = q_right.shape[0]
    slice_rows = q_left.shape[1]
    halves = n_dp // 2
    shared = [tokens * parts // 16 // n_mp // 16 * 16 for parts in SHARED]
    direct = [tokens - rows * n_mp for rows in shared]

    def at_dp(index):
        return (index, mp)

    def at_mp(index):
        return (dp, index)

    partner = at_dp(group * 4 + places[1])
    across = at_dp(group * 4 + places[2])

    def group_at(s):
        return lax.rem(group + s, groups)

    def peer(s):
        return at_dp(group_at(s) * 4 + place)

    def remote(src, dst, send, recv, device):
        return pltpu.make_async_remote_copy(
            src_ref=src,
            dst_ref=dst,
            send_sem=send,
            recv_sem=recv,
            device_id=device,
            device_id_type=pl.DeviceIdType.MESH,
        )

    barrier = pltpu.get_barrier_semaphore()
    friends = [partner, across]
    friends += [peer(s) for s in range(1, groups)]
    friends += [at_mp(lax.rem(mp + m, n_mp)) for m in range(1, n_mp)]
    for friend in friends:
        pl.semaphore_signal(barrier, inc=1, device_id=friend, device_id_type=pl.DeviceIdType.MESH)
    pl.semaphore_wait(barrier, len(friends))

    sends = []

    def go(copy):
        copy.start()
        sends.append(copy)

    def piece(p, size):
        if size == width and not isinstance(p, int):
            return pl.ds(pl.multiple_of(p * width, width), width)
        return pl.ds(p * width if p < wide else wide * width + (p - wide) * 128, size)

    def size_of(p):
        return width if p < wide else ends[p - wide]

    def basis_across(p, size):
        return remote(
            out_basis.at[:, piece(p, size)],
            basis.at[pl.ds(2 * depth, depth), piece(p, size)],
            bx_s.at[p],
            bx_r.at[p],
            across,
        )

    def basis_forward(p, size):
        return remote(
            basis.at[pl.ds(2 * depth, depth), piece(p, size)],
            basis.at[pl.ds(3 * depth, depth), piece(p, size)],
            bf_s.at[p],
            bf_r.at[p],
            partner,
        )

    basis_partner = remote(
        out_basis, basis.at[pl.ds(depth, depth), :], bd_s.at[0], bd_r.at[0], partner
    )

    def grads_over(s, q, rows, send, recv):
        start = (group_at(s) * 4 + places[q]) * depth
        return remote(
            grads.at[rows, pl.ds(pl.multiple_of(start, 128), depth)],
            peer_g.at[s - 1, rows, pl.ds(q * depth, depth)],
            send,
            recv,
            peer(s),
        )

    def share_rows(q, plane):
        return pl.ds(pl.multiple_of(direct[q] + plane * shared[q], 16), shared[q])

    chunks = [(s, q) for s in range(1, groups) for q in range(4)]

    def grads_shared(e):
        s, q = chunks[e]
        return grads_over(s, q, share_rows(q, mp), gs_s.at[e], gs_r.at[e])

    def grads_direct(e):
        s, q = chunks[e]
        return grads_over(s, q, pl.ds(0, direct[q]), gd_s.at[e], gd_r.at[e])

    def share(e, plane):
        s, q = chunks[e]
        return peer_g.at[s - 1, share_rows(q, plane), pl.ds(q * depth, depth)]

    def relay_up(e, r):
        ref = share(e, mp - r)
        return remote(ref, ref, zr_s.at[e, r], zr_r.at[e, r], at_mp(mp + 1))

    def relay_down(e, r):
        ref = share(e, mp + r)
        return remote(ref, ref, zl_s.at[e, r], zl_r.at[e, r], at_mp(mp - 1))

    def from_below(e, r):
        ref = share(e, mp - r)
        return remote(ref, ref, zr_s.at[e, r - 1], zr_r.at[e, r - 1], at_mp(mp - 1))

    def from_above(e, r):
        ref = share(e, mp + r)
        return remote(ref, ref, zl_s.at[e, r - 1], zl_r.at[e, r - 1], at_mp(mp + 1))

    core = lax.rem(place, 2)

    def right_across():
        return remote(q_right, right.at[core, 1], qx_s.at[0], qx_r.at[0], across)

    def right_over(s, j):
        slot = (s - 1) * 2 + j
        return remote(
            q_right if j == 0 else right.at[core, 1],
            right.at[core, s * 2 + j],
            qy_s.at[slot],
            qy_r.at[slot],
            peer(s),
        )

    def right_partner():
        return remote(right.at[core], right.at[core], qd_s.at[0], qd_r.at[0], partner)

    def right_arrived_partner():
        return remote(right.at[1 - core], right.at[1 - core], qd_s.at[0], qd_r.at[0], partner)

    def left_across():
        return remote(q_left.at[mp], left.at[mp, core, 1], lx_s.at[0], lx_r.at[0], across)

    def left_over(s, j):
        slot = (s - 1) * 2 + j
        return remote(
            q_left.at[mp] if j == 0 else left.at[mp, core, 1],
            left.at[mp, core, s * 2 + j],
            ly_s.at[slot],
            ly_r.at[slot],
            peer(s),
        )

    def left_partner(plane):
        rows = left.at[plane, core]
        return remote(rows, rows, ld_s.at[plane], ld_r.at[plane], partner)

    def left_arrived_partner(plane):
        rows = left.at[plane, 1 - core]
        return remote(rows, rows, ld_s.at[plane], ld_r.at[plane], partner)

    items = 2

    def item(i, plane):
        if i == 0:
            return rin.at[pl.ds(pl.multiple_of(plane * in_cols, in_cols), in_cols), :]
        return left.at[plane, core, pl.ds(1, halves - 1)]

    def item_up(i, r):
        ref = item(i, mp - r)
        return remote(ref, ref, iu_s.at[i, r], iu_r.at[i, r], at_mp(mp + 1))

    def item_down(i, r):
        ref = item(i, mp + r)
        return remote(ref, ref, id_s.at[i, r], id_r.at[i, r], at_mp(mp - 1))

    def item_below(i, r):
        ref = item(i, mp - r)
        return remote(ref, ref, iu_s.at[i, r - 1], iu_r.at[i, r - 1], at_mp(mp - 1))

    def item_above(i, r):
        ref = item(i, mp + r)
        return remote(ref, ref, id_s.at[i, r - 1], id_r.at[i, r - 1], at_mp(mp + 1))

    go(left_across())
    for e in range(len(chunks)):
        go(grads_shared(e))
    for s in range(1, groups):
        go(left_over(s, 0))
    for p in range(2):
        go(basis_across(p, size_of(p)))
    go(right_across())
    for p in range(2, pieces):
        go(basis_across(p, size_of(p)))
    go(basis_partner)

    k_chunks = acts.shape[1] // act_buf.shape[2]
    k_size = act_buf.shape[2]

    def load_chunk(i):
        slot = i % 2
        return (
            pltpu.make_async_copy(
                acts.at[:, pl.ds(i * k_size, k_size)], act_buf.at[slot], chunk_sem.at[slot, 0]
            ),
            pltpu.make_async_copy(
                in_basis.at[pl.ds(i * k_size, k_size), :], inb_buf.at[slot], chunk_sem.at[slot, 1]
            ),
        )

    for copy in load_chunk(0):
        copy.start()
    loads = [pltpu.make_async_copy(out_basis, basis.at[pl.ds(0, depth), :], load_sem.at[0])]
    for q in range(4):
        start = (group * 4 + places[q]) * depth
        loads.append(
            pltpu.make_async_copy(
                grads.at[:, pl.ds(pl.multiple_of(start, 128), depth)],
                own_g.at[:, pl.ds(q * depth, depth)],
                load_sem.at[1 + q],
            )
        )
    loads.append(pltpu.make_async_copy(q_left, left.at[:, core, 0], load_sem.at[5]))
    loads.append(pltpu.make_async_copy(q_right, right.at[core, 0], load_sem.at[6]))
    for copy in loads:
        copy.start()

    def load_eig(p):
        slot = p % 2 if isinstance(p, int) else lax.rem(p, 2)
        return pltpu.make_async_copy(eigen.at[:, piece(p, width)], eig.at[slot], eig_sem.at[slot])

    load_eig(0).start()

    for i in range(k_chunks):
        if i + 1 < k_chunks:
            for copy in load_chunk(i + 1):
                copy.start()
        for copy in load_chunk(i):
            copy.wait()
        term = jnp.dot(act_buf[i % 2], inb_buf[i % 2], preferred_element_type=jnp.float32)
        if i == 0:
            acc[:, :in_cols] = term
        else:
            acc[:, :in_cols] += term
    rin_rows = pl.ds(pl.multiple_of(mp * in_cols, in_cols), in_cols)
    rin[rin_rows, :] = jnp.transpose(acc[:, :in_cols]).astype(jnp.bfloat16)

    def weigh():
        live = length[0, 0]
        active_row = lax.broadcasted_iota(jnp.int32, (1, tokens), 1) < live
        active_col = lax.broadcasted_iota(jnp.int32, (tokens, 1), 0) < live
        columns = jnp.broadcast_to(ids[...], (tokens, tokens))
        same = (jnp.transpose(columns) == columns) & active_row
        repeats = jnp.sum(jnp.where(same, 1.0, 0.0), axis=1, keepdims=True)
        weight[...] = jnp.where(active_col, 1.0 / jnp.maximum(repeats, 1.0), 0.0)
        sums[...] = jnp.zeros_like(sums)

    left_across().wait_recv()
    for s in range(1, groups):
        go(left_over(s, 1))
    for e in range(len(chunks)):
        go(grads_direct(e))
    for s in range(1, groups):
        go(right_over(s, 0))

    def up_if(r):
        return (mp >= r) & (mp < n_mp - 1)

    def down_if(r):
        return (mp + r <= n_mp - 1) & (mp > 0)

    for step in range(len(chunks) + n_mp - 2):
        if step < len(chunks):
            grads_shared(step).wait_recv()
        for r in range(n_mp - 1):
            e = step - r
            if not 0 <= e < len(chunks):
                continue

            @pl.when(up_if(r))
            def _():
                if r > 0:
                    from_below(e, r).wait_recv()
                relay_up(e, r).start()

            @pl.when(down_if(r))
            def _():
                if r > 0:
                    from_above(e, r).wait_recv()
                relay_down(e, r).start()

        if step == 0:
            weigh()

    def relay_items(r):
        @pl.when(up_if(r))
        def _():
            for i in range(items):
                if r > 0:
                    item_below(i, r).wait_recv()
                item_up(i, r).start()

        @pl.when(down_if(r))
        def _():
            for i in range(items):
                if r > 0:
                    item_above(i, r).wait_recv()
                item_down(i, r).start()

    for s in range(1, groups):
        for j in range(2):
            left_over(s, j).wait_recv()
    relay_items(0)

    def relay_right():
        right_across().wait_recv()
        for s in range(1, groups):
            right_over(s, 1).start()

    for copy in loads:
        copy.wait()
    basis_partner.wait_recv()

    def part_over(s, p, size):
        return remote(
            part_out.at[s - 1, :, piece(p, size)],
            part_in.at[s - 1, :, piece(p, size)],
            ss_s.at[s - 1, p],
            ss_r.at[s - 1, p],
            peer(groups - s),
        )

    def term(rows, p, size, first, count):
        k = pl.ds(first * depth, count * depth)
        return jnp.dot(rows[:, k], basis[k, piece(p, size)], preferred_element_type=jnp.float32)

    def room(j, size):
        return pl.ds(j * width, size)

    def own(p, size):
        mine = room(0, size)
        basis_across(p, size).wait_recv()
        basis_forward(p, size).start()
        acc[:, mine] = term(own_g, p, size, 0, 3)
        basis_forward(p, size).wait_recv()
        total = acc[:, mine] + term(own_g, p, size, 3, 1)
        own_out[:, piece(p, size)] = total.astype(jnp.bfloat16)

    def parts(p, size):
        for j in range(groups - 1):
            total = term(peer_g.at[j], p, size, 0, 4)
            part_out[j, :, piece(p, size)] = total.astype(jnp.bfloat16)
            part_over(j + 1, p, size).start()

    rows_from = [peer_g.at[s - 1] for s in range(1, groups)] + [own_g]

    def rotate(p, size):
        basis_across(p, size).wait_recv()
        basis_forward(p, size).start()
        for j, rows in enumerate(rows_from):
            acc[:, room(j, size)] = term(rows, p, size, 0, 3)
        basis_forward(p, size).wait_recv()
        for j, rows in enumerate(rows_from):
            total = acc[:, room(j, size)] + term(rows, p, size, 3, 1)
            finish(j, p, size, total)

    def finish(j, p, size, total):
        if j < groups - 1:
            part_out[j, :, piece(p, size)] = total.astype(jnp.bfloat16)
            part_over(j + 1, p, size).start()
        else:
            own_out[:, piece(p, size)] = total.astype(jnp.bfloat16)

    def prepare():
        for j, rows in enumerate(rows_from):
            acc_end[:, room(j, width)] = term(rows, wide, width, 0, 2)

    def rotate_end(t):
        p, size = wide + t, ends[t]
        basis_across(p, size).wait_recv()
        basis_forward(p, size).start()
        for j, rows in enumerate(rows_from):
            acc_end[:, pl.ds(j * width + t * 128, size)] += term(rows, p, size, 2, 1)
        basis_forward(p, size).wait_recv()
        for j, rows in enumerate(rows_from):
            total = acc_end[:, pl.ds(j * width + t * 128, size)] + term(rows, p, size, 3, 1)
            finish(j, p, size, total)

    def right_arrives():
        for s in range(1, groups):
            for j in range(2):
                right_over(s, j).wait_recv()
        right_partner().start()
        left_partner(mp).start()

    def left_arrives(r):
        @pl.when(mp >= r)
        def _():
            @pl.when(mp == n_mp - 1)
            def _():
                for i in range(items):
                    item_below(i, r).wait_recv()

            left_partner(mp - r).start()

        @pl.when(mp + r <= n_mp - 1)
        def _():
            @pl.when(mp == 0)
            def _():
                for i in range(items):
                    item_above(i, r).wait_recv()

            left_partner(mp + r).start()

    def factors_arrive():
        for plane in range(n_mp):
            left_arrived_partner(plane).wait_recv()
        right_arrived_partner().wait_recv()

    def score(p, size):
        last = isinstance(p, int)
        load_eig(p).wait()
        if not last:
            load_eig(p + 1).start()
        total = own_out[:, piece(p, size)].astype(jnp.float32)
        for s in range(1, groups):
            if last:
                for t in range(len(ends)):
                    part_over(s, wide + t, ends[t]).wait_recv()
            else:
                part_over(s, p, size).wait_recv()
            total = total + part_in[s - 1, :, piece(p, size)].astype(jnp.float32)
        rotated = total.astype(jnp.bfloat16).astype(jnp.float32)
        scaled = (weight[...] * rotated).astype(jnp.bfloat16)
        slot = p % 2 if last else lax.rem(p, 2)
        block = 512
        for i in range(0, kin, block):
            rows = pl.ds(i, block)
            gradient = jnp.dot(rin[rows, :], scaled, preferred_element_type=jnp.float32)
            denominator = eig[slot, rows, :].astype(jnp.float32) + damping
            cond[rows, :] = (gradient / denominator).astype(jnp.bfloat16)
        for plane in range(n_mp):
            lhs = left[plane].reshape(n_dp * slice_rows, kin)
            factor = right[:, :, pl.ds(plane * slice_rows, slice_rows), piece(p, size)]
            mixture = jnp.dot(lhs, cond[...], preferred_element_type=jnp.float32)
            weighted = mixture * factor.reshape(n_dp * slice_rows, size).astype(jnp.float32)
            folded = weighted[:, :128]
            for c in range(128, size, 128):
                folded = folded + weighted[:, c : c + 128]
            sums[plane] += folded

    def first(p, carry):
        @pl.when(p == early - 1)
        def _():
            relay_right()
            relay_items(1)

        own(p, width)
        return carry

    lax.fori_loop(0, early, first, 0)

    for e in range(len(chunks)):
        grads_direct(e).wait_recv()
        for r in range(1, n_mp):

            @pl.when((mp >= r) & (mp == n_mp - 1))
            def _():
                from_below(e, r).wait_recv()

            @pl.when((mp + r <= n_mp - 1) & (mp == 0))
            def _():
                from_above(e, r).wait_recv()

    for r in range(2, n_mp - 1):
        relay_items(r)

    def scored(p):
        done = jnp.where(p < wide - 1, 0, jnp.where(p == wide + 1, wide, p - wide + 4))
        return jnp.minimum(done, wide)

    def one(i, carry):
        score(i, width)
        return carry

    def step(p, carry):
        @pl.when(p < early)
        def _():
            parts(p, width)

        @pl.when((p >= early) & (p < wide))
        def _():
            rotate(p, width)

        for t in range(len(ends)):

            @pl.when(p == wide + t)
            def _():
                rotate_end(t)

        @pl.when(p == wide - 2)
        def _():
            right_arrives()
            for r in range(1, n_mp - 1):
                left_arrives(r)
            prepare()

        @pl.when(p == wide - 1)
        def _():
            left_arrives(n_mp - 1)
            factors_arrive()

        lax.fori_loop(scored(p - 1), scored(p), one, 0)
        return carry

    lax.fori_loop(0, pieces, step, 0)
    lax.fori_loop(scored(pieces - 1), wide, one, 0)
    score(wide, width)

    per_block = out.shape[1] // n_dp
    rank = q_rows // per_block
    unit = min(rank, slice_rows)
    totals = {}
    for plane in range(n_mp):
        for u in range(slice_rows // unit):
            local = (plane * slice_rows + u * unit) // rank
            block = sums[plane].reshape(n_dp, slice_rows, 128)[:, u * unit : (u + 1) * unit, :]
            found = jnp.sum(block, axis=1)
            totals[local] = totals[local] + found if local in totals else found
    for s in range(groups):
        for j in range(2):
            for c in range(2):
                chip = lax.div(places[2 * j], 2)
                block = (group_at(groups - s) * 4 + chip * 2 + c) * per_block
                at = c * halves + s * 2 + j
                for local, found in totals.items():
                    gathered[0, pl.ds(block + local, 1), :] = found[at : at + 1, :]

    def score_over(m):
        return remote(
            gathered.at[0],
            gathered.at[m],
            sc_s.at[m],
            sc_r.at[m],
            at_mp(lax.rem(mp + m, n_mp)),
        )

    for m in range(1, n_mp):
        go(score_over(m))
    for copy in sends:
        copy.wait_send()
    for r in range(n_mp - 1):

        @pl.when(up_if(r))
        def _():
            for i in range(items):
                item_up(i, r).wait_send()

        @pl.when(down_if(r))
        def _():
            for i in range(items):
                item_down(i, r).wait_send()

    for s in range(1, groups):
        right_over(s, 1).wait_send()
    right_partner().wait_send()
    for plane in range(n_mp):
        left_partner(plane).wait_send()

    def sent(p, size):
        basis_forward(p, size).wait_send()
        for s in range(1, groups):
            part_over(s, p, size).wait_send()

    for p in range(pieces):
        sent(p, size_of(p))
    for e in range(len(chunks)):
        for r in range(n_mp - 1):

            @pl.when(up_if(r))
            def _():
                relay_up(e, r).wait_send()

            @pl.when(down_if(r))
            def _():
                relay_down(e, r).wait_send()

    total = gathered[0]
    for m in range(1, n_mp):
        score_over(m).wait_recv()
        total = total + gathered[m]
    out[...] = jnp.sum(jnp.transpose(total), axis=0, keepdims=True)

def per_device(
    n_dp,
    n_mp,
    doc_ids,
    doc_lengths,
    activations,
    out_grads,
    input_basis,
    output_basis,
    eigenvalues,
    query_left,
    query_right,
):
    groups = n_dp // 4
    tokens = out_grads.shape[0]
    depth, cols = output_basis.shape
    kin = eigenvalues.shape[0]
    in_cols = input_basis.shape[1]
    per_block, rank = query_left.shape[:2]
    q_rows = per_block * rank
    queries = n_dp * per_block
    width, wide, ends = piece_plan(cols)
    pieces = wide + len(ends)
    chunks = (groups - 1) * 4
    k_size = 512
    bf16, f32 = jnp.bfloat16, jnp.float32

    def pair(*shape):
        return [pltpu.SemaphoreType.DMA(shape), pltpu.SemaphoreType.DMA(shape)]

    vmem = pl.BlockSpec(memory_space=pltpu.VMEM)
    hbm = pl.BlockSpec(memory_space=pl.ANY)
    summed = pl.pallas_call(
        functools.partial(kernel, n_dp, n_mp),
        out_shape=jax.ShapeDtypeStruct((1, queries), f32),
        in_specs=[vmem, pl.BlockSpec(memory_space=pltpu.SMEM)] + [hbm] * 7,
        out_specs=vmem,
        scratch_shapes=[
            pltpu.VMEM((4 * depth, cols), bf16),
            pltpu.VMEM((tokens, 4 * depth), bf16),
            pltpu.VMEM((groups - 1, tokens, 4 * depth), bf16),
            pltpu.VMEM((kin, tokens), bf16),
            pltpu.VMEM((n_mp, 2, n_dp // 2, q_rows // n_mp, kin), bf16),
            pltpu.VMEM((2, n_dp // 2, q_rows, cols), bf16),
            pltpu.VMEM((2, kin, width), bf16),
            pltpu.VMEM((groups - 1, tokens, cols), bf16),
            pltpu.VMEM((groups - 1, tokens, cols), bf16),
            pltpu.VMEM((tokens, cols), bf16),
            pltpu.VMEM((2, tokens, k_size), bf16),
            pltpu.VMEM((2, k_size, in_cols), bf16),
            pltpu.VMEM((tokens, max(in_cols, groups * width)), f32),
            pltpu.VMEM((tokens, groups * width), f32),
            pltpu.VMEM((kin, width), bf16),
            pltpu.VMEM((tokens, 1), f32),
            pltpu.VMEM((n_mp, n_dp * q_rows // n_mp, 128), f32),
            pltpu.VMEM((n_mp, queries, 128), f32),
            pltpu.SemaphoreType.DMA((7,)),
            pltpu.SemaphoreType.DMA((2, 2)),
            pltpu.SemaphoreType.DMA((2,)),
            *pair(pieces),
            *pair(1),
            *pair(pieces),
            *pair(chunks),
            *pair(chunks),
            *pair(chunks, n_mp - 1),
            *pair(chunks, n_mp - 1),
            *pair(1),
            *pair((groups - 1) * 2),
            *pair(1),
            *pair(1),
            *pair((groups - 1) * 2),
            *pair(2, n_mp - 1),
            *pair(2, n_mp - 1),
            *pair(n_mp),
            *pair(groups - 1, pieces),
            *pair(n_mp),
        ],
        compiler_params=pltpu.CompilerParams(
            collective_id=0, has_side_effects=True, vmem_limit_bytes=67043328
        ),
    )(
        doc_ids,
        doc_lengths.reshape(1, 1),
        activations,
        out_grads,
        input_basis,
        output_basis,
        eigenvalues,
        query_left.reshape(n_mp, q_rows // n_mp, kin),
        query_right.reshape(q_rows, cols),
    )
    return summed


def solution(mesh):
    return jax.shard_map(
        functools.partial(per_device, mesh.shape["dp"], mesh.shape["mp"]),
        mesh=mesh,
        in_specs=(
            P("dp", None),
            P("dp"),
            P("dp", None),
            P("dp", None),
            P(None, "mp"),
            P("dp", "mp"),
            P(None, "mp"),
            P("dp", None, None),
            P("dp", None, "mp"),
        ),
        out_specs=P("dp", None),
        check_vma=False,
    )
```

```python
import functools

import jax
import jax.numpy as jnp
from jax import lax
from jax.experimental import pallas as pl
from jax.experimental.pallas import tpu as pltpu
from jax.sharding import PartitionSpec as P

damping = 0.5
EARLY = 3
SHARED = (8, 8, 10, 10)


def piece_plan(columns):
    width = 256 if columns % 256 == 0 else 128
    return width, columns // width - 1, [128] * (width // 128)


def kernel(
    n_dp,
    n_mp,
    ids,
    length,
    acts,
    grads,
    in_basis,
    out_basis,
    eigen,
    q_left,
    q_right,
    out,
    basis,
    own_g,
    peer_g,
    rin,
    left,
    right,
    eig,
    part_out,
    part_in,
    own_out,
    act_buf,
    inb_buf,
    acc,
    acc_end,
    cond,
    weight,
    sums,
    gathered,
    load_sem,
    chunk_sem,
    eig_sem,
    bx_s,
    bx_r,
    bd_s,
    bd_r,
    bf_s,
    bf_r,
    gs_s,
    gs_r,
    gd_s,
    gd_r,
    zr_s,
    zr_r,
    zl_s,
    zl_r,
    qx_s,
    qx_r,
    qy_s,
    qy_r,
    qd_s,
    qd_r,
    lx_s,
    lx_r,
    ly_s,
    ly_r,
    iu_s,
    iu_r,
    id_s,
    id_r,
    ld_s,
    ld_r,
    ss_s,
    ss_r,
    sc_s,
    sc_r,
):
    groups = n_dp // 4
    dp, mp = lax.axis_index("dp"), lax.axis_index("mp")
    group, place = lax.div(dp, 4), lax.rem(dp, 4)
    places = (place, place + 1 - 2 * lax.rem(place, 2), lax.rem(place + 2, 4), 3 - place)

    tokens = grads.shape[0]
    depth, cols = out_basis.shape
    width, wide, ends = piece_plan(cols)
    pieces = wide + len(ends)
    early = min(EARLY, wide)
    in_cols = in_basis.shape[1]
    kin = rin.shape[0]
    q_rows = q_right.shape[0]
    slice_rows = q_left.shape[1]
    halves = n_dp // 2
    shared = [tokens * parts // 16 // n_mp // 16 * 16 for parts in SHARED]
    direct = [tokens - rows * n_mp for rows in shared]

    def at_dp(index):
        return (index, mp)

    def at_mp(index):
        return (dp, index)

    partner = at_dp(group * 4 + places[1])
    across = at_dp(group * 4 + places[2])

    def group_at(s):
        return lax.rem(group + s, groups)

    def peer(s):
        return at_dp(group_at(s) * 4 + place)

    def remote(src, dst, send, recv, device):
        return pltpu.make_async_remote_copy(
            src_ref=src,
            dst_ref=dst,
            send_sem=send,
            recv_sem=recv,
            device_id=device,
            device_id_type=pl.DeviceIdType.MESH,
        )

    barrier = pltpu.get_barrier_semaphore()
    friends = [partner, across]
    friends += [peer(s) for s in range(1, groups)]

    def greet(friend):
        pl.semaphore_signal(barrier, inc=1, device_id=friend, device_id_type=pl.DeviceIdType.MESH)

    for friend in friends:
        greet(friend)
    below, above = mp > 0, mp < n_mp - 1

    @pl.when(below)
    def _():
        greet(at_mp(mp - 1))

    @pl.when(above)
    def _():
        greet(at_mp(mp + 1))

    pl.semaphore_wait(barrier, len(friends) + below.astype(jnp.int32) + above.astype(jnp.int32))

    sends = []

    def go(copy):
        copy.start()
        sends.append(copy)

    def piece(p, size):
        if size == width and not isinstance(p, int):
            return pl.ds(pl.multiple_of(p * width, width), width)
        return pl.ds(p * width if p < wide else wide * width + (p - wide) * 128, size)

    def size_of(p):
        return width if p < wide else ends[p - wide]

    def basis_across(p, size):
        return remote(
            out_basis.at[:, piece(p, size)],
            basis.at[pl.ds(2 * depth, depth), piece(p, size)],
            bx_s.at[p],
            bx_r.at[p],
            across,
        )

    half = depth // 2

    def last_across(h):
        p = pieces - 1
        columns = piece(p, ends[-1])
        return remote(
            out_basis.at[pl.ds(h * half, half), columns],
            basis.at[pl.ds(2 * depth + h * half, half), columns],
            bx_s.at[p + h],
            bx_r.at[p + h],
            across,
        )

    def last_forward(h):
        p = pieces - 1
        columns = piece(p, ends[-1])
        return remote(
            basis.at[pl.ds(2 * depth + h * half, half), columns],
            basis.at[pl.ds(3 * depth + h * half, half), columns],
            bf_s.at[p + h],
            bf_r.at[p + h],
            partner,
        )

    def basis_forward(p, size):
        return remote(
            basis.at[pl.ds(2 * depth, depth), piece(p, size)],
            basis.at[pl.ds(3 * depth, depth), piece(p, size)],
            bf_s.at[p],
            bf_r.at[p],
            partner,
        )

    basis_partner = remote(
        out_basis, basis.at[pl.ds(depth, depth), :], bd_s.at[0], bd_r.at[0], partner
    )

    def grads_over(s, q, rows, send, recv):
        start = (group_at(s) * 4 + places[q]) * depth
        return remote(
            grads.at[rows, pl.ds(pl.multiple_of(start, 128), depth)],
            peer_g.at[s - 1, rows, pl.ds(q * depth, depth)],
            send,
            recv,
            peer(s),
        )

    def share_rows(q, plane):
        return pl.ds(pl.multiple_of(direct[q] + plane * shared[q], 16), shared[q])

    chunks = [(s, q) for s in range(1, groups) for q in range(4)]

    def grads_shared(e):
        s, q = chunks[e]
        return grads_over(s, q, share_rows(q, mp), gs_s.at[e], gs_r.at[e])

    def grads_direct(e):
        s, q = chunks[e]
        return grads_over(s, q, pl.ds(0, direct[q]), gd_s.at[e], gd_r.at[e])

    def share(e, plane):
        s, q = chunks[e]
        return peer_g.at[s - 1, share_rows(q, plane), pl.ds(q * depth, depth)]

    def relay_up(e, r):
        ref = share(e, mp - r)
        return remote(ref, ref, zr_s.at[e, r], zr_r.at[e, r], at_mp(mp + 1))

    def relay_down(e, r):
        ref = share(e, mp + r)
        return remote(ref, ref, zl_s.at[e, r], zl_r.at[e, r], at_mp(mp - 1))

    def from_below(e, r):
        ref = share(e, mp - r)
        return remote(ref, ref, zr_s.at[e, r - 1], zr_r.at[e, r - 1], at_mp(mp - 1))

    def from_above(e, r):
        ref = share(e, mp + r)
        return remote(ref, ref, zl_s.at[e, r - 1], zl_r.at[e, r - 1], at_mp(mp + 1))

    core = lax.rem(place, 2)

    def right_across():
        return remote(q_right, right.at[core, 1], qx_s.at[0], qx_r.at[0], across)

    def right_over(s, j):
        slot = (s - 1) * 2 + j
        return remote(
            q_right if j == 0 else right.at[core, 1],
            right.at[core, s * 2 + j],
            qy_s.at[slot],
            qy_r.at[slot],
            peer(s),
        )

    def right_partner():
        return remote(right.at[core], right.at[core], qd_s.at[0], qd_r.at[0], partner)

    def right_arrived_partner():
        return remote(right.at[1 - core], right.at[1 - core], qd_s.at[0], qd_r.at[0], partner)

    def left_across():
        return remote(q_left.at[mp], left.at[mp, core, 1], lx_s.at[0], lx_r.at[0], across)

    def left_over(s, j):
        slot = (s - 1) * 2 + j
        return remote(
            q_left.at[mp] if j == 0 else left.at[mp, core, 1],
            left.at[mp, core, s * 2 + j],
            ly_s.at[slot],
            ly_r.at[slot],
            peer(s),
        )

    def left_partner(plane):
        rows = left.at[plane, core]
        return remote(rows, rows, ld_s.at[plane], ld_r.at[plane], partner)

    def left_arrived_partner(plane):
        rows = left.at[plane, 1 - core]
        return remote(rows, rows, ld_s.at[plane], ld_r.at[plane], partner)

    items = 2

    def item(i, plane):
        if i == 0:
            return rin.at[pl.ds(pl.multiple_of(plane * in_cols, in_cols), in_cols), :]
        return left.at[plane, core, pl.ds(1, halves - 1)]

    def item_up(i, r):
        ref = item(i, mp - r)
        return remote(ref, ref, iu_s.at[i, r], iu_r.at[i, r], at_mp(mp + 1))

    def item_down(i, r):
        ref = item(i, mp + r)
        return remote(ref, ref, id_s.at[i, r], id_r.at[i, r], at_mp(mp - 1))

    def item_below(i, r):
        ref = item(i, mp - r)
        return remote(ref, ref, iu_s.at[i, r - 1], iu_r.at[i, r - 1], at_mp(mp - 1))

    def item_above(i, r):
        ref = item(i, mp + r)
        return remote(ref, ref, id_s.at[i, r - 1], id_r.at[i, r - 1], at_mp(mp + 1))

    go(left_across())
    for e in range(len(chunks)):
        go(grads_shared(e))
    for s in range(1, groups):
        go(left_over(s, 0))
    for p in range(2):
        go(basis_across(p, size_of(p)))
    go(right_across())
    for p in range(2, pieces - 1):
        go(basis_across(p, size_of(p)))
    for h in range(2):
        go(last_across(h))
    go(basis_partner)

    k_chunks = acts.shape[1] // act_buf.shape[2]
    k_size = act_buf.shape[2]

    def load_chunk(i):
        slot = i % 2
        return (
            pltpu.make_async_copy(
                acts.at[:, pl.ds(i * k_size, k_size)], act_buf.at[slot], chunk_sem.at[slot, 0]
            ),
            pltpu.make_async_copy(
                in_basis.at[pl.ds(i * k_size, k_size), :], inb_buf.at[slot], chunk_sem.at[slot, 1]
            ),
        )

    for copy in load_chunk(0):
        copy.start()
    loads = [pltpu.make_async_copy(out_basis, basis.at[pl.ds(0, depth), :], load_sem.at[0])]
    for q in range(4):
        start = (group * 4 + places[q]) * depth
        loads.append(
            pltpu.make_async_copy(
                grads.at[:, pl.ds(pl.multiple_of(start, 128), depth)],
                own_g.at[:, pl.ds(q * depth, depth)],
                load_sem.at[1 + q],
            )
        )
    loads.append(pltpu.make_async_copy(q_left, left.at[:, core, 0], load_sem.at[5]))
    loads.append(pltpu.make_async_copy(q_right, right.at[core, 0], load_sem.at[6]))
    for copy in loads:
        copy.start()

    def load_eig(p):
        slot = p % 2 if isinstance(p, int) else lax.rem(p, 2)
        return pltpu.make_async_copy(eigen.at[:, piece(p, width)], eig.at[slot], eig_sem.at[slot])

    load_eig(0).start()

    for i in range(k_chunks):
        if i + 1 < k_chunks:
            for copy in load_chunk(i + 1):
                copy.start()
        for copy in load_chunk(i):
            copy.wait()
        term = jnp.dot(act_buf[i % 2], inb_buf[i % 2], preferred_element_type=jnp.float32)
        if i == 0:
            acc[:, :in_cols] = term
        else:
            acc[:, :in_cols] += term
    rin_rows = pl.ds(pl.multiple_of(mp * in_cols, in_cols), in_cols)
    rin[rin_rows, :] = jnp.transpose(acc[:, :in_cols]).astype(jnp.bfloat16)

    def weigh():
        live = length[0, 0]
        active_row = lax.broadcasted_iota(jnp.int32, (1, tokens), 1) < live
        active_col = lax.broadcasted_iota(jnp.int32, (tokens, 1), 0) < live
        columns = jnp.broadcast_to(ids[...], (tokens, tokens))
        same = (jnp.transpose(columns) == columns) & active_row
        repeats = jnp.sum(jnp.where(same, 1.0, 0.0), axis=1, keepdims=True)
        weight[...] = jnp.where(active_col, 1.0 / jnp.maximum(repeats, 1.0), 0.0)
        sums[...] = jnp.zeros_like(sums)

    left_across().wait_recv()
    for s in range(1, groups):
        go(left_over(s, 1))
    for e in range(len(chunks)):
        go(grads_direct(e))
    for s in range(1, groups):
        go(right_over(s, 0))

    def up_if(r):
        return (mp >= r) & (mp < n_mp - 1)

    def down_if(r):
        return (mp + r <= n_mp - 1) & (mp > 0)

    for step in range(len(chunks) + n_mp - 2):
        if step < len(chunks):
            grads_shared(step).wait_recv()
        for r in range(n_mp - 1):
            e = step - r
            if not 0 <= e < len(chunks):
                continue

            @pl.when(up_if(r))
            def _():
                if r > 0:
                    from_below(e, r).wait_recv()
                relay_up(e, r).start()

            @pl.when(down_if(r))
            def _():
                if r > 0:
                    from_above(e, r).wait_recv()
                relay_down(e, r).start()

        if step == 0:
            weigh()

    def relay_items(r):
        @pl.when(up_if(r))
        def _():
            for i in range(items):
                if r > 0:
                    item_below(i, r).wait_recv()
                item_up(i, r).start()

        @pl.when(down_if(r))
        def _():
            for i in range(items):
                if r > 0:
                    item_above(i, r).wait_recv()
                item_down(i, r).start()

    for s in range(1, groups):
        for j in range(2):
            left_over(s, j).wait_recv()
    relay_items(0)

    def relay_right():
        right_across().wait_recv()
        for s in range(1, groups):
            right_over(s, 1).start()

    for copy in loads:
        copy.wait()
    basis_partner.wait_recv()

    def part_over(s, p, size):
        return remote(
            part_out.at[s - 1, :, piece(p, size)],
            part_in.at[s - 1, :, piece(p, size)],
            ss_s.at[s - 1, p],
            ss_r.at[s - 1, p],
            peer(groups - s),
        )

    def term(rows, p, size, first, count):
        k = pl.ds(first * depth, count * depth)
        return jnp.dot(rows[:, k], basis[k, piece(p, size)], preferred_element_type=jnp.float32)

    def room(j, size):
        return pl.ds(j * width, size)

    def own(p, size):
        mine = room(0, size)
        basis_across(p, size).wait_recv()
        basis_forward(p, size).start()
        acc[:, mine] = term(own_g, p, size, 0, 3)
        basis_forward(p, size).wait_recv()
        total = acc[:, mine] + term(own_g, p, size, 3, 1)
        own_out[:, piece(p, size)] = total.astype(jnp.bfloat16)

    def parts(p, size):
        for j in range(groups - 1):
            total = term(peer_g.at[j], p, size, 0, 4)
            part_out[j, :, piece(p, size)] = total.astype(jnp.bfloat16)
            part_over(j + 1, p, size).start()

    rows_from = [peer_g.at[s - 1] for s in range(1, groups)] + [own_g]

    def rotate(p, size):
        for j, rows in enumerate(rows_from):
            acc[:, room(j, size)] = term(rows, p, size, 0, 2)
        basis_across(p, size).wait_recv()
        basis_forward(p, size).start()
        for j, rows in enumerate(rows_from):
            acc[:, room(j, size)] += term(rows, p, size, 2, 1)
        basis_forward(p, size).wait_recv()
        for j, rows in enumerate(rows_from):
            total = acc[:, room(j, size)] + term(rows, p, size, 3, 1)
            finish(j, p, size, total)

    def finish(j, p, size, total):
        if j < groups - 1:
            part_out[j, :, piece(p, size)] = total.astype(jnp.bfloat16)
            part_over(j + 1, p, size).start()
        else:
            own_out[:, piece(p, size)] = total.astype(jnp.bfloat16)

    def prepare():
        for j, rows in enumerate(rows_from):
            acc_end[:, room(j, width)] = term(rows, wide, width, 0, 2)

    def start_end(t):
        p, size = wide + t, ends[t]
        if p == pieces - 1:
            for h in range(2):
                last_across(h).wait_recv()
                last_forward(h).start()
        else:
            basis_across(p, size).wait_recv()
            basis_forward(p, size).start()

    def finish_end(t):
        p, size = wide + t, ends[t]
        here = [pl.ds(j * width + t * 128, size) for j in range(groups)]
        for j in range(groups - 1):
            acc_end[:, here[j]] += term(rows_from[j], p, size, 2, 1)
        if p == pieces - 1:
            for h in range(2):
                last_forward(h).wait_recv()
        else:
            basis_forward(p, size).wait_recv()
        for j in range(groups - 1):
            finish(j, p, size, acc_end[:, here[j]] + term(rows_from[j], p, size, 3, 1))
        j = groups - 1
        finish(j, p, size, acc_end[:, here[j]] + term(rows_from[j], p, size, 2, 2))

    def right_arrives():
        for s in range(1, groups):
            for j in range(2):
                right_over(s, j).wait_recv()
        right_partner().start()
        left_partner(mp).start()

    def left_arrives(r):
        @pl.when(mp >= r)
        def _():
            @pl.when(mp == n_mp - 1)
            def _():
                for i in range(items):
                    item_below(i, r).wait_recv()

            left_partner(mp - r).start()

        @pl.when(mp + r <= n_mp - 1)
        def _():
            @pl.when(mp == 0)
            def _():
                for i in range(items):
                    item_above(i, r).wait_recv()

            left_partner(mp + r).start()

    def factors_arrive():
        for plane in range(n_mp):
            left_arrived_partner(plane).wait_recv()
        right_arrived_partner().wait_recv()

    block = 512

    def condition(slot, p, size, first):
        total = own_out[:, piece(p, size)].astype(jnp.float32)
        for s in range(1, groups):
            part_over(s, p, size).wait_recv()
            total = total + part_in[s - 1, :, piece(p, size)].astype(jnp.float32)
        rotated = total.astype(jnp.bfloat16).astype(jnp.float32)
        scaled = (weight[...] * rotated).astype(jnp.bfloat16)
        place_in = pl.ds(first, size)
        for i in range(0, kin, block):
            rows = pl.ds(i, block)
            gradient = jnp.dot(rin[rows, :], scaled, preferred_element_type=jnp.float32)
            denominator = eig[slot, rows, place_in].astype(jnp.float32) + damping
            cond[rows, place_in] = (gradient / denominator).astype(jnp.bfloat16)

    def mix(p):
        for plane in range(n_mp):
            lhs = left[plane].reshape(n_dp * slice_rows, kin)
            factor = right[:, :, pl.ds(plane * slice_rows, slice_rows), piece(p, width)]
            mixture = jnp.dot(lhs, cond[...], preferred_element_type=jnp.float32)
            weighted = mixture * factor.reshape(n_dp * slice_rows, width).astype(jnp.float32)
            folded = weighted[:, :128]
            for c in range(128, width, 128):
                folded = folded + weighted[:, c : c + 128]
            sums[plane] += folded

    def score(p):
        load_eig(p).wait()
        load_eig(p + 1).start()
        condition(lax.rem(p, 2), p, width, 0)
        mix(p)

    def score_ends():
        load_eig(wide).wait()
        for t, size in enumerate(ends):
            condition(wide % 2, wide + t, size, t * 128)
        mix(wide)

    def first(p, carry):
        @pl.when(p == early - 1)
        def _():
            relay_right()
            relay_items(1)

        own(p, width)
        return carry

    lax.fori_loop(0, early, first, 0)

    for e in range(len(chunks)):
        grads_direct(e).wait_recv()
        for r in range(1, n_mp):

            @pl.when((mp >= r) & (mp == n_mp - 1))
            def _():
                from_below(e, r).wait_recv()

            @pl.when((mp + r <= n_mp - 1) & (mp == 0))
            def _():
                from_above(e, r).wait_recv()

    for r in range(2, n_mp - 1):
        relay_items(r)

    def scored(p):
        done = jnp.where(p < wide - 1, 0, jnp.where(p > wide, wide, 3 * (p - wide) + 5))
        return jnp.minimum(done, wide)

    def one(i, carry):
        score(i)
        return carry

    def step(p, carry):
        @pl.when(p < early)
        def _():
            parts(p, width)

        @pl.when((p >= early) & (p < wide))
        def _():
            rotate(p, width)

        for t in range(len(ends)):

            @pl.when(p == wide + t)
            def _():
                if t == 0:
                    one(2, 0)
                else:
                    start_end(t)
                finish_end(t)

        @pl.when(p == wide - 2)
        def _():
            right_arrives()
            for r in range(1, n_mp - 1):
                left_arrives(r)
            prepare()

        @pl.when(p == wide - 1)
        def _():
            left_arrives(n_mp - 1)
            factors_arrive()

        first = scored(p - 1) + jnp.where(p == wide, 1, 0)
        lax.fori_loop(first, scored(p), one, 0)

        @pl.when(p == wide - 1)
        def _():
            start_end(0)

        return carry

    lax.fori_loop(0, pieces, step, 0)
    lax.fori_loop(scored(pieces - 1), wide, one, 0)
    score_ends()

    per_block = out.shape[1] // n_dp
    rank = q_rows // per_block
    unit = min(rank, slice_rows)
    totals = {}
    for plane in range(n_mp):
        for u in range(slice_rows // unit):
            local = (plane * slice_rows + u * unit) // rank
            block = sums[plane].reshape(n_dp, slice_rows, 128)[:, u * unit : (u + 1) * unit, :]
            found = jnp.sum(block, axis=1)
            totals[local] = totals[local] + found if local in totals else found
    for s in range(groups):
        for j in range(2):
            for c in range(2):
                chip = lax.div(places[2 * j], 2)
                block = (group_at(groups - s) * 4 + chip * 2 + c) * per_block
                at = c * halves + s * 2 + j
                for local, found in totals.items():
                    gathered[0, pl.ds(block + local, 1), :] = found[at : at + 1, :]

    def score_over(m):
        return remote(
            gathered.at[0],
            gathered.at[m],
            sc_s.at[m],
            sc_r.at[m],
            at_mp(lax.rem(mp + m, n_mp)),
        )

    for m in range(1, n_mp):
        go(score_over(m))
    for copy in sends:
        copy.wait_send()
    for r in range(n_mp - 1):

        @pl.when(up_if(r))
        def _():
            for i in range(items):
                item_up(i, r).wait_send()

        @pl.when(down_if(r))
        def _():
            for i in range(items):
                item_down(i, r).wait_send()

    for s in range(1, groups):
        right_over(s, 1).wait_send()
    right_partner().wait_send()
    for plane in range(n_mp):
        left_partner(plane).wait_send()

    def sent(p, size):
        if p < pieces - 1:
            basis_forward(p, size).wait_send()
        else:
            for h in range(2):
                last_forward(h).wait_send()
        for s in range(1, groups):
            part_over(s, p, size).wait_send()

    for p in range(pieces):
        sent(p, size_of(p))
    for e in range(len(chunks)):
        for r in range(n_mp - 1):

            @pl.when(up_if(r))
            def _():
                relay_up(e, r).wait_send()

            @pl.when(down_if(r))
            def _():
                relay_down(e, r).wait_send()

    total = gathered[0]
    for m in range(1, n_mp):
        score_over(m).wait_recv()
        total = total + gathered[m]
    out[...] = jnp.sum(jnp.transpose(total), axis=0, keepdims=True)

def per_device(
    n_dp,
    n_mp,
    doc_ids,
    doc_lengths,
    activations,
    out_grads,
    input_basis,
    output_basis,
    eigenvalues,
    query_left,
    query_right,
):
    groups = n_dp // 4
    tokens = out_grads.shape[0]
    depth, cols = output_basis.shape
    kin = eigenvalues.shape[0]
    in_cols = input_basis.shape[1]
    per_block, rank = query_left.shape[:2]
    q_rows = per_block * rank
    queries = n_dp * per_block
    width, wide, ends = piece_plan(cols)
    pieces = wide + len(ends)
    chunks = (groups - 1) * 4
    k_size = 512
    bf16, f32 = jnp.bfloat16, jnp.float32

    def pair(*shape):
        return [pltpu.SemaphoreType.DMA(shape), pltpu.SemaphoreType.DMA(shape)]

    vmem = pl.BlockSpec(memory_space=pltpu.VMEM)
    hbm = pl.BlockSpec(memory_space=pl.ANY)
    summed = pl.pallas_call(
        functools.partial(kernel, n_dp, n_mp),
        out_shape=jax.ShapeDtypeStruct((1, queries), f32),
        in_specs=[vmem, pl.BlockSpec(memory_space=pltpu.SMEM)] + [hbm] * 7,
        out_specs=vmem,
        scratch_shapes=[
            pltpu.VMEM((4 * depth, cols), bf16),
            pltpu.VMEM((tokens, 4 * depth), bf16),
            pltpu.VMEM((groups - 1, tokens, 4 * depth), bf16),
            pltpu.VMEM((kin, tokens), bf16),
            pltpu.VMEM((n_mp, 2, n_dp // 2, q_rows // n_mp, kin), bf16),
            pltpu.VMEM((2, n_dp // 2, q_rows, cols), bf16),
            pltpu.VMEM((2, kin, width), bf16),
            pltpu.VMEM((groups - 1, tokens, cols), bf16),
            pltpu.VMEM((groups - 1, tokens, cols), bf16),
            pltpu.VMEM((tokens, cols), bf16),
            pltpu.VMEM((2, tokens, k_size), bf16),
            pltpu.VMEM((2, k_size, in_cols), bf16),
            pltpu.VMEM((tokens, max(in_cols, groups * width)), f32),
            pltpu.VMEM((tokens, groups * width), f32),
            pltpu.VMEM((kin, width), bf16),
            pltpu.VMEM((tokens, 1), f32),
            pltpu.VMEM((n_mp, n_dp * q_rows // n_mp, 128), f32),
            pltpu.VMEM((n_mp, queries, 128), f32),
            pltpu.SemaphoreType.DMA((7,)),
            pltpu.SemaphoreType.DMA((2, 2)),
            pltpu.SemaphoreType.DMA((2,)),
            *pair(pieces + 1),
            *pair(1),
            *pair(pieces + 1),
            *pair(chunks),
            *pair(chunks),
            *pair(chunks, n_mp - 1),
            *pair(chunks, n_mp - 1),
            *pair(1),
            *pair((groups - 1) * 2),
            *pair(1),
            *pair(1),
            *pair((groups - 1) * 2),
            *pair(2, n_mp - 1),
            *pair(2, n_mp - 1),
            *pair(n_mp),
            *pair(groups - 1, pieces),
            *pair(n_mp),
        ],
        compiler_params=pltpu.CompilerParams(
            collective_id=0, has_side_effects=True, vmem_limit_bytes=67043328
        ),
    )(
        doc_ids,
        doc_lengths.reshape(1, 1),
        activations,
        out_grads,
        input_basis,
        output_basis,
        eigenvalues,
        query_left.reshape(n_mp, q_rows // n_mp, kin),
        query_right.reshape(q_rows, cols),
    )
    return summed


def solution(mesh):
    return jax.shard_map(
        functools.partial(per_device, mesh.shape["dp"], mesh.shape["mp"]),
        mesh=mesh,
        in_specs=(
            P("dp", None),
            P("dp"),
            P("dp", None),
            P("dp", None),
            P(None, "mp"),
            P("dp", "mp"),
            P(None, "mp"),
            P("dp", None, None),
            P("dp", None, "mp"),
        ),
        out_specs=P("dp", None),
        check_vma=False,
    )
```

```python
import functools

import jax
import jax.numpy as jnp
from jax import lax
from jax.experimental import pallas as pl
from jax.experimental.pallas import tpu as pltpu
from jax.sharding import PartitionSpec as P

damping = 0.5
EARLY = 3
SHARED = (8, 8, 10, 10)


def piece_plan(columns):
    width = 256 if columns % 256 == 0 else 128
    return width, columns // width - 1, [128] * (width // 128)


def kernel(
    n_dp,
    n_mp,
    ids,
    length,
    acts,
    grads,
    in_basis,
    out_basis,
    eigen,
    q_left,
    q_right,
    out,
    basis,
    own_g,
    peer_g,
    rin,
    left,
    right,
    eig,
    part_out,
    part_in,
    own_out,
    act_buf,
    inb_buf,
    acc,
    acc_end,
    cond,
    weight,
    sums,
    gathered,
    load_sem,
    chunk_sem,
    eig_sem,
    bx_s,
    bx_r,
    bd_s,
    bd_r,
    bf_s,
    bf_r,
    gs_s,
    gs_r,
    gd_s,
    gd_r,
    zr_s,
    zr_r,
    zl_s,
    zl_r,
    qx_s,
    qx_r,
    qy_s,
    qy_r,
    qd_s,
    qd_r,
    lx_s,
    lx_r,
    ly_s,
    ly_r,
    iu_s,
    iu_r,
    id_s,
    id_r,
    ld_s,
    ld_r,
    ss_s,
    ss_r,
    sc_s,
    sc_r,
):
    groups = n_dp // 4
    dp, mp = lax.axis_index("dp"), lax.axis_index("mp")
    group, place = lax.div(dp, 4), lax.rem(dp, 4)
    places = (place, place + 1 - 2 * lax.rem(place, 2), lax.rem(place + 2, 4), 3 - place)

    tokens = grads.shape[0]
    depth, cols = out_basis.shape
    width, wide, ends = piece_plan(cols)
    pieces = wide + len(ends)
    early = min(EARLY, wide)
    in_cols = in_basis.shape[1]
    kin = rin.shape[0]
    q_rows = q_right.shape[0]
    slice_rows = q_left.shape[1]
    halves = n_dp // 2
    shared = [tokens * parts // 16 // n_mp // 16 * 16 for parts in SHARED]
    direct = [tokens - rows * n_mp for rows in shared]

    def at_dp(index):
        return (index, mp)

    def at_mp(index):
        return (dp, index)

    partner = at_dp(group * 4 + places[1])
    across = at_dp(group * 4 + places[2])

    def group_at(s):
        return lax.rem(group + s, groups)

    def peer(s):
        return at_dp(group_at(s) * 4 + place)

    def remote(src, dst, send, recv, device):
        return pltpu.make_async_remote_copy(
            src_ref=src,
            dst_ref=dst,
            send_sem=send,
            recv_sem=recv,
            device_id=device,
            device_id_type=pl.DeviceIdType.MESH,
        )

    barrier = pltpu.get_barrier_semaphore()
    friends = [partner, across]
    friends += [peer(s) for s in range(1, groups)]

    def greet(friend):
        pl.semaphore_signal(barrier, inc=1, device_id=friend, device_id_type=pl.DeviceIdType.MESH)

    for friend in friends:
        greet(friend)
    below, above = mp > 0, mp < n_mp - 1

    @pl.when(below)
    def _():
        greet(at_mp(mp - 1))

    @pl.when(above)
    def _():
        greet(at_mp(mp + 1))

    pl.semaphore_wait(barrier, len(friends) + below.astype(jnp.int32) + above.astype(jnp.int32))

    sends = []

    def go(copy):
        copy.start()
        sends.append(copy)

    def piece(p, size):
        if size == width and not isinstance(p, int):
            return pl.ds(pl.multiple_of(p * width, width), width)
        return pl.ds(p * width if p < wide else wide * width + (p - wide) * 128, size)

    def size_of(p):
        return width if p < wide else ends[p - wide]

    def basis_across(p, size):
        return remote(
            out_basis.at[:, piece(p, size)],
            basis.at[pl.ds(2 * depth, depth), piece(p, size)],
            bx_s.at[p],
            bx_r.at[p],
            across,
        )

    half = depth // 2

    def last_across(h):
        p = pieces - 1
        columns = piece(p, ends[-1])
        return remote(
            out_basis.at[pl.ds(h * half, half), columns],
            basis.at[pl.ds(2 * depth + h * half, half), columns],
            bx_s.at[p + h],
            bx_r.at[p + h],
            across,
        )

    def last_forward(h):
        p = pieces - 1
        columns = piece(p, ends[-1])
        return remote(
            basis.at[pl.ds(2 * depth + h * half, half), columns],
            basis.at[pl.ds(3 * depth + h * half, half), columns],
            bf_s.at[p + h],
            bf_r.at[p + h],
            partner,
        )

    def basis_forward(p, size):
        return remote(
            basis.at[pl.ds(2 * depth, depth), piece(p, size)],
            basis.at[pl.ds(3 * depth, depth), piece(p, size)],
            bf_s.at[p],
            bf_r.at[p],
            partner,
        )

    basis_partner = remote(
        out_basis, basis.at[pl.ds(depth, depth), :], bd_s.at[0], bd_r.at[0], partner
    )

    def grads_over(s, q, rows, send, recv):
        start = (group_at(s) * 4 + places[q]) * depth
        return remote(
            grads.at[rows, pl.ds(pl.multiple_of(start, 128), depth)],
            peer_g.at[s - 1, rows, pl.ds(q * depth, depth)],
            send,
            recv,
            peer(s),
        )

    def share_rows(q, plane):
        return pl.ds(pl.multiple_of(direct[q] + plane * shared[q], 16), shared[q])

    chunks = [(s, q) for s in range(1, groups) for q in range(4)]

    def grads_shared(e):
        s, q = chunks[e]
        return grads_over(s, q, share_rows(q, mp), gs_s.at[e], gs_r.at[e])

    def grads_direct(e):
        s, q = chunks[e]
        return grads_over(s, q, pl.ds(0, direct[q]), gd_s.at[e], gd_r.at[e])

    def share(e, plane):
        s, q = chunks[e]
        return peer_g.at[s - 1, share_rows(q, plane), pl.ds(q * depth, depth)]

    def relay_up(e, r):
        ref = share(e, mp - r)
        return remote(ref, ref, zr_s.at[e, r], zr_r.at[e, r], at_mp(mp + 1))

    def relay_down(e, r):
        ref = share(e, mp + r)
        return remote(ref, ref, zl_s.at[e, r], zl_r.at[e, r], at_mp(mp - 1))

    def from_below(e, r):
        ref = share(e, mp - r)
        return remote(ref, ref, zr_s.at[e, r - 1], zr_r.at[e, r - 1], at_mp(mp - 1))

    def from_above(e, r):
        ref = share(e, mp + r)
        return remote(ref, ref, zl_s.at[e, r - 1], zl_r.at[e, r - 1], at_mp(mp + 1))

    core = lax.rem(place, 2)

    def right_across():
        return remote(q_right, right.at[core, 1], qx_s.at[0], qx_r.at[0], across)

    def right_over(s, j):
        slot = (s - 1) * 2 + j
        return remote(
            q_right if j == 0 else right.at[core, 1],
            right.at[core, s * 2 + j],
            qy_s.at[slot],
            qy_r.at[slot],
            peer(s),
        )

    def right_partner():
        return remote(right.at[core], right.at[core], qd_s.at[0], qd_r.at[0], partner)

    def right_arrived_partner():
        return remote(right.at[1 - core], right.at[1 - core], qd_s.at[0], qd_r.at[0], partner)

    def left_across():
        return remote(q_left.at[mp], left.at[mp, core, 1], lx_s.at[0], lx_r.at[0], across)

    def left_over(s, j):
        slot = (s - 1) * 2 + j
        return remote(
            q_left.at[mp] if j == 0 else left.at[mp, core, 1],
            left.at[mp, core, s * 2 + j],
            ly_s.at[slot],
            ly_r.at[slot],
            peer(s),
        )

    def left_partner(plane):
        rows = left.at[plane, core]
        return remote(rows, rows, ld_s.at[plane], ld_r.at[plane], partner)

    def left_arrived_partner(plane):
        rows = left.at[plane, 1 - core]
        return remote(rows, rows, ld_s.at[plane], ld_r.at[plane], partner)

    items = 2

    def item(i, plane):
        if i == 0:
            return rin.at[pl.ds(pl.multiple_of(plane * in_cols, in_cols), in_cols), :]
        return left.at[plane, core, pl.ds(1, halves - 1)]

    def item_up(i, r):
        ref = item(i, mp - r)
        return remote(ref, ref, iu_s.at[i, r], iu_r.at[i, r], at_mp(mp + 1))

    def item_down(i, r):
        ref = item(i, mp + r)
        return remote(ref, ref, id_s.at[i, r], id_r.at[i, r], at_mp(mp - 1))

    def item_below(i, r):
        ref = item(i, mp - r)
        return remote(ref, ref, iu_s.at[i, r - 1], iu_r.at[i, r - 1], at_mp(mp - 1))

    def item_above(i, r):
        ref = item(i, mp + r)
        return remote(ref, ref, id_s.at[i, r - 1], id_r.at[i, r - 1], at_mp(mp + 1))

    go(left_across())
    for e in range(len(chunks)):
        go(grads_shared(e))
    for s in range(1, groups):
        go(left_over(s, 0))
    for p in range(2):
        go(basis_across(p, size_of(p)))
    go(right_across())
    for p in range(2, pieces - 1):
        go(basis_across(p, size_of(p)))
    for h in range(2):
        go(last_across(h))
    go(basis_partner)

    k_chunks = acts.shape[1] // act_buf.shape[2]
    k_size = act_buf.shape[2]

    def load_chunk(i):
        slot = i % 2
        return (
            pltpu.make_async_copy(
                acts.at[:, pl.ds(i * k_size, k_size)], act_buf.at[slot], chunk_sem.at[slot, 0]
            ),
            pltpu.make_async_copy(
                in_basis.at[pl.ds(i * k_size, k_size), :], inb_buf.at[slot], chunk_sem.at[slot, 1]
            ),
        )

    for copy in load_chunk(0):
        copy.start()
    loads = [pltpu.make_async_copy(out_basis, basis.at[pl.ds(0, depth), :], load_sem.at[0])]
    for q in range(4):
        start = (group * 4 + places[q]) * depth
        loads.append(
            pltpu.make_async_copy(
                grads.at[:, pl.ds(pl.multiple_of(start, 128), depth)],
                own_g.at[:, pl.ds(q * depth, depth)],
                load_sem.at[1 + q],
            )
        )
    loads.append(pltpu.make_async_copy(q_left, left.at[:, core, 0], load_sem.at[5]))
    loads.append(pltpu.make_async_copy(q_right, right.at[core, 0], load_sem.at[6]))
    for copy in loads:
        copy.start()

    def load_eig(p):
        slot = p % 2 if isinstance(p, int) else lax.rem(p, 2)
        return pltpu.make_async_copy(eigen.at[:, piece(p, width)], eig.at[slot], eig_sem.at[slot])

    load_eig(0).start()

    for i in range(k_chunks):
        if i + 1 < k_chunks:
            for copy in load_chunk(i + 1):
                copy.start()
        for copy in load_chunk(i):
            copy.wait()
        term = jnp.dot(act_buf[i % 2], inb_buf[i % 2], preferred_element_type=jnp.float32)
        if i == 0:
            acc[:, :in_cols] = term
        else:
            acc[:, :in_cols] += term
    rin_rows = pl.ds(pl.multiple_of(mp * in_cols, in_cols), in_cols)
    rin[rin_rows, :] = jnp.transpose(acc[:, :in_cols]).astype(jnp.bfloat16)

    def weigh():
        live = length[0, 0]
        active_row = lax.broadcasted_iota(jnp.int32, (1, tokens), 1) < live
        active_col = lax.broadcasted_iota(jnp.int32, (tokens, 1), 0) < live
        columns = jnp.broadcast_to(ids[...], (tokens, tokens))
        same = (jnp.transpose(columns) == columns) & active_row
        repeats = jnp.sum(jnp.where(same, 1.0, 0.0), axis=1, keepdims=True)
        weight[...] = jnp.where(active_col, 1.0 / jnp.maximum(repeats, 1.0), 0.0)
        sums[...] = jnp.zeros_like(sums)

    left_across().wait_recv()
    for s in range(1, groups):
        go(left_over(s, 1))
    for e in range(len(chunks)):
        go(grads_direct(e))
    for s in range(1, groups):
        go(right_over(s, 0))

    def up_if(r):
        return (mp >= r) & (mp < n_mp - 1)

    def down_if(r):
        return (mp + r <= n_mp - 1) & (mp > 0)

    for step in range(len(chunks) + n_mp - 2):
        if step < len(chunks):
            grads_shared(step).wait_recv()
        for r in range(n_mp - 1):
            e = step - r
            if not 0 <= e < len(chunks):
                continue

            @pl.when(up_if(r))
            def _():
                if r > 0:
                    from_below(e, r).wait_recv()
                relay_up(e, r).start()

            @pl.when(down_if(r))
            def _():
                if r > 0:
                    from_above(e, r).wait_recv()
                relay_down(e, r).start()

        if step == 0:
            weigh()

    def relay_items(r):
        @pl.when(up_if(r))
        def _():
            for i in range(items):
                if r > 0:
                    item_below(i, r).wait_recv()
                item_up(i, r).start()

        @pl.when(down_if(r))
        def _():
            for i in range(items):
                if r > 0:
                    item_above(i, r).wait_recv()
                item_down(i, r).start()

    for s in range(1, groups):
        for j in range(2):
            left_over(s, j).wait_recv()
    relay_items(0)

    def relay_right():
        right_across().wait_recv()
        for s in range(1, groups):
            right_over(s, 1).start()

    for copy in loads:
        copy.wait()
    basis_partner.wait_recv()

    def part_over(s, p, size):
        return remote(
            part_out.at[s - 1, :, piece(p, size)],
            part_in.at[s - 1, :, piece(p, size)],
            ss_s.at[s - 1, p],
            ss_r.at[s - 1, p],
            peer(groups - s),
        )

    def term(rows, p, size, first, count):
        k = pl.ds(first * depth, count * depth)
        return jnp.dot(rows[:, k], basis[k, piece(p, size)], preferred_element_type=jnp.float32)

    def room(j, size):
        return pl.ds(j * width, size)

    def own(p, size):
        mine = room(0, size)
        basis_across(p, size).wait_recv()
        basis_forward(p, size).start()
        acc[:, mine] = term(own_g, p, size, 0, 3)
        basis_forward(p, size).wait_recv()
        total = acc[:, mine] + term(own_g, p, size, 3, 1)
        own_out[:, piece(p, size)] = total.astype(jnp.bfloat16)

    def parts(p, size):
        for j in range(groups - 1):
            total = term(peer_g.at[j], p, size, 0, 4)
            part_out[j, :, piece(p, size)] = total.astype(jnp.bfloat16)
            part_over(j + 1, p, size).start()

    rows_from = [peer_g.at[s - 1] for s in range(1, groups)] + [own_g]

    def rotate(p, size):
        for j, rows in enumerate(rows_from):
            acc[:, room(j, size)] = term(rows, p, size, 0, 2)
        basis_across(p, size).wait_recv()
        basis_forward(p, size).start()
        for j, rows in enumerate(rows_from):
            acc[:, room(j, size)] += term(rows, p, size, 2, 1)
        basis_forward(p, size).wait_recv()
        for j, rows in enumerate(rows_from):
            total = acc[:, room(j, size)] + term(rows, p, size, 3, 1)
            finish(j, p, size, total)

    def finish(j, p, size, total):
        if j < groups - 1:
            part_out[j, :, piece(p, size)] = total.astype(jnp.bfloat16)
            part_over(j + 1, p, size).start()
        else:
            own_out[:, piece(p, size)] = total.astype(jnp.bfloat16)

    def prepare():
        for j, rows in enumerate(rows_from):
            acc_end[:, room(j, width)] = term(rows, wide, width, 0, 2)

    def start_end(t):
        p, size = wide + t, ends[t]
        if p == pieces - 1:
            for h in range(2):
                last_across(h).wait_recv()
                last_forward(h).start()
        else:
            basis_across(p, size).wait_recv()
            basis_forward(p, size).start()

    def finish_end(t):
        p, size = wide + t, ends[t]
        here = [pl.ds(j * width + t * 128, size) for j in range(groups)]
        for j in range(groups - 1):
            acc_end[:, here[j]] += term(rows_from[j], p, size, 2, 1)
        if p == pieces - 1:
            for h in range(2):
                last_forward(h).wait_recv()
        else:
            basis_forward(p, size).wait_recv()
        for j in range(groups - 1):
            finish(j, p, size, acc_end[:, here[j]] + term(rows_from[j], p, size, 3, 1))
        j = groups - 1
        finish(j, p, size, acc_end[:, here[j]] + term(rows_from[j], p, size, 2, 2))

    def right_arrives():
        for s in range(1, groups):
            for j in range(2):
                right_over(s, j).wait_recv()
        right_partner().start()
        left_partner(mp).start()

    def left_arrives(r):
        @pl.when(mp >= r)
        def _():
            @pl.when(mp == n_mp - 1)
            def _():
                for i in range(items):
                    item_below(i, r).wait_recv()

            left_partner(mp - r).start()

        @pl.when(mp + r <= n_mp - 1)
        def _():
            @pl.when(mp == 0)
            def _():
                for i in range(items):
                    item_above(i, r).wait_recv()

            left_partner(mp + r).start()

    def factors_arrive():
        for plane in range(n_mp):
            left_arrived_partner(plane).wait_recv()
        right_arrived_partner().wait_recv()

    block = min(1024, kin)

    def condition(slot, p, size, first):
        total = own_out[:, piece(p, size)].astype(jnp.float32)
        for s in range(1, groups):
            part_over(s, p, size).wait_recv()
            total = total + part_in[s - 1, :, piece(p, size)].astype(jnp.float32)
        rotated = total.astype(jnp.bfloat16).astype(jnp.float32)
        scaled = (weight[...] * rotated).astype(jnp.bfloat16)
        place_in = pl.ds(first, size)
        for i in range(0, kin, block):
            rows = pl.ds(i, block)
            gradient = jnp.dot(rin[rows, :], scaled, preferred_element_type=jnp.float32)
            denominator = eig[slot, rows, place_in].astype(jnp.float32) + damping
            cond[rows, place_in] = (gradient / denominator).astype(jnp.bfloat16)

    def mix(p):
        for plane in range(n_mp):
            lhs = left[plane].reshape(n_dp * slice_rows, kin)
            factor = right[:, :, pl.ds(plane * slice_rows, slice_rows), piece(p, width)]
            mixture = jnp.dot(lhs, cond[...], preferred_element_type=jnp.float32)
            weighted = mixture * factor.reshape(n_dp * slice_rows, width).astype(jnp.float32)
            folded = weighted[:, :128]
            for c in range(128, width, 128):
                folded = folded + weighted[:, c : c + 128]
            sums[plane] += folded

    def score(p):
        load_eig(p).wait()
        load_eig(p + 1).start()
        condition(lax.rem(p, 2), p, width, 0)
        mix(p)

    def score_ends():
        load_eig(wide).wait()
        for t, size in enumerate(ends):
            condition(wide % 2, wide + t, size, t * 128)
        mix(wide)

    def first(p, carry):
        @pl.when(p == early - 1)
        def _():
            relay_right()
            relay_items(1)

        own(p, width)
        return carry

    lax.fori_loop(0, early, first, 0)

    for e in range(len(chunks)):
        grads_direct(e).wait_recv()
        for r in range(1, n_mp):

            @pl.when((mp >= r) & (mp == n_mp - 1))
            def _():
                from_below(e, r).wait_recv()

            @pl.when((mp + r <= n_mp - 1) & (mp == 0))
            def _():
                from_above(e, r).wait_recv()

    for r in range(2, n_mp - 1):
        relay_items(r)

    def scored(p):
        done = jnp.where(p < wide - 1, 0, jnp.where(p > wide, wide, 3 * (p - wide) + 5))
        return jnp.minimum(done, wide)

    def one(i, carry):
        score(i)
        return carry

    def step(p, carry):
        @pl.when(p < early)
        def _():
            parts(p, width)

        @pl.when((p >= early) & (p < wide))
        def _():
            rotate(p, width)

        for t in range(len(ends)):

            @pl.when(p == wide + t)
            def _():
                if t == 0:
                    one(2, 0)
                else:
                    start_end(t)
                finish_end(t)

        @pl.when(p == wide - 2)
        def _():
            right_arrives()
            for r in range(1, n_mp - 1):
                left_arrives(r)
            prepare()

        @pl.when(p == wide - 1)
        def _():
            left_arrives(n_mp - 1)
            factors_arrive()

        first = scored(p - 1) + jnp.where(p == wide, 1, 0)
        lax.fori_loop(first, scored(p), one, 0)

        @pl.when(p == wide - 1)
        def _():
            start_end(0)

        return carry

    lax.fori_loop(0, pieces, step, 0)
    lax.fori_loop(scored(pieces - 1), wide, one, 0)
    score_ends()

    per_block = out.shape[1] // n_dp
    rank = q_rows // per_block
    unit = min(rank, slice_rows)
    totals = {}
    for plane in range(n_mp):
        for u in range(slice_rows // unit):
            local = (plane * slice_rows + u * unit) // rank
            block = sums[plane].reshape(n_dp, slice_rows, 128)[:, u * unit : (u + 1) * unit, :]
            found = jnp.sum(block, axis=1)
            totals[local] = totals[local] + found if local in totals else found
    for s in range(groups):
        for j in range(2):
            for c in range(2):
                chip = lax.div(places[2 * j], 2)
                block = (group_at(groups - s) * 4 + chip * 2 + c) * per_block
                at = c * halves + s * 2 + j
                for local, found in totals.items():
                    gathered[0, pl.ds(block + local, 1), :] = found[at : at + 1, :]

    def score_over(m):
        return remote(
            gathered.at[0],
            gathered.at[m],
            sc_s.at[m],
            sc_r.at[m],
            at_mp(lax.rem(mp + m, n_mp)),
        )

    for m in range(1, n_mp):
        go(score_over(m))
    for copy in sends:
        copy.wait_send()
    for r in range(n_mp - 1):

        @pl.when(up_if(r))
        def _():
            for i in range(items):
                item_up(i, r).wait_send()

        @pl.when(down_if(r))
        def _():
            for i in range(items):
                item_down(i, r).wait_send()

    for s in range(1, groups):
        right_over(s, 1).wait_send()
    right_partner().wait_send()
    for plane in range(n_mp):
        left_partner(plane).wait_send()

    def sent(p, size):
        if p < pieces - 1:
            basis_forward(p, size).wait_send()
        else:
            for h in range(2):
                last_forward(h).wait_send()
        for s in range(1, groups):
            part_over(s, p, size).wait_send()

    for p in range(pieces):
        sent(p, size_of(p))
    for e in range(len(chunks)):
        for r in range(n_mp - 1):

            @pl.when(up_if(r))
            def _():
                relay_up(e, r).wait_send()

            @pl.when(down_if(r))
            def _():
                relay_down(e, r).wait_send()

    total = gathered[0]
    for m in range(1, n_mp):
        score_over(m).wait_recv()
        total = total + gathered[m]
    out[...] = jnp.sum(jnp.transpose(total), axis=0, keepdims=True)

def per_device(
    n_dp,
    n_mp,
    doc_ids,
    doc_lengths,
    activations,
    out_grads,
    input_basis,
    output_basis,
    eigenvalues,
    query_left,
    query_right,
):
    groups = n_dp // 4
    tokens = out_grads.shape[0]
    depth, cols = output_basis.shape
    kin = eigenvalues.shape[0]
    in_cols = input_basis.shape[1]
    per_block, rank = query_left.shape[:2]
    q_rows = per_block * rank
    queries = n_dp * per_block
    width, wide, ends = piece_plan(cols)
    pieces = wide + len(ends)
    chunks = (groups - 1) * 4
    k_size = 512
    bf16, f32 = jnp.bfloat16, jnp.float32

    def pair(*shape):
        return [pltpu.SemaphoreType.DMA(shape), pltpu.SemaphoreType.DMA(shape)]

    vmem = pl.BlockSpec(memory_space=pltpu.VMEM)
    hbm = pl.BlockSpec(memory_space=pl.ANY)
    summed = pl.pallas_call(
        functools.partial(kernel, n_dp, n_mp),
        out_shape=jax.ShapeDtypeStruct((1, queries), f32),
        in_specs=[vmem, pl.BlockSpec(memory_space=pltpu.SMEM)] + [hbm] * 7,
        out_specs=vmem,
        scratch_shapes=[
            pltpu.VMEM((4 * depth, cols), bf16),
            pltpu.VMEM((tokens, 4 * depth), bf16),
            pltpu.VMEM((groups - 1, tokens, 4 * depth), bf16),
            pltpu.VMEM((kin, tokens), bf16),
            pltpu.VMEM((n_mp, 2, n_dp // 2, q_rows // n_mp, kin), bf16),
            pltpu.VMEM((2, n_dp // 2, q_rows, cols), bf16),
            pltpu.VMEM((2, kin, width), bf16),
            pltpu.VMEM((groups - 1, tokens, cols), bf16),
            pltpu.VMEM((groups - 1, tokens, cols), bf16),
            pltpu.VMEM((tokens, cols), bf16),
            pltpu.VMEM((2, tokens, k_size), bf16),
            pltpu.VMEM((2, k_size, in_cols), bf16),
            pltpu.VMEM((tokens, max(in_cols, groups * width)), f32),
            pltpu.VMEM((tokens, groups * width), f32),
            pltpu.VMEM((kin, width), bf16),
            pltpu.VMEM((tokens, 1), f32),
            pltpu.VMEM((n_mp, n_dp * q_rows // n_mp, 128), f32),
            pltpu.VMEM((n_mp, queries, 128), f32),
            pltpu.SemaphoreType.DMA((7,)),
            pltpu.SemaphoreType.DMA((2, 2)),
            pltpu.SemaphoreType.DMA((2,)),
            *pair(pieces + 1),
            *pair(1),
            *pair(pieces + 1),
            *pair(chunks),
            *pair(chunks),
            *pair(chunks, n_mp - 1),
            *pair(chunks, n_mp - 1),
            *pair(1),
            *pair((groups - 1) * 2),
            *pair(1),
            *pair(1),
            *pair((groups - 1) * 2),
            *pair(2, n_mp - 1),
            *pair(2, n_mp - 1),
            *pair(n_mp),
            *pair(groups - 1, pieces),
            *pair(n_mp),
        ],
        compiler_params=pltpu.CompilerParams(
            collective_id=0, has_side_effects=True, vmem_limit_bytes=67043328
        ),
    )(
        doc_ids,
        doc_lengths.reshape(1, 1),
        activations,
        out_grads,
        input_basis,
        output_basis,
        eigenvalues,
        query_left.reshape(n_mp, q_rows // n_mp, kin),
        query_right.reshape(q_rows, cols),
    )
    return summed


def solution(mesh):
    return jax.shard_map(
        functools.partial(per_device, mesh.shape["dp"], mesh.shape["mp"]),
        mesh=mesh,
        in_specs=(
            P("dp", None),
            P("dp"),
            P("dp", None),
            P("dp", None),
            P(None, "mp"),
            P("dp", "mp"),
            P(None, "mp"),
            P("dp", None, None),
            P("dp", None, "mp"),
        ),
        out_specs=P("dp", None),
        check_vma=False,
    )
```
